128 devices in a mesh: section: 2 (over core), dev: 64 (over x, z, y).
Axes of the slice: x: 4, y: 4, z: 4, core: 2. Of those that a mesh axis runs over, the one named last changes fastest.
Arguments:
- indices: int32 [8192, 32, 8], P(('section', 'dev')), may hold values from 0 to 131071
- pool_len: int32 [32], replicated, may hold values from 1 to 8
- tables: bfloat16 [4194304, 128], P(('section', 'dev')), may hold values from -3 to 3
- w_first: bfloat16 [4096, 4096], P('dev', 'section'), may hold values from -0.09375 to 0.09375
- b_first: bfloat16 [4096], P('section'), may hold values from -3 to 3
- w_out: bfloat16 [4096], P('section'), may hold values from -0.09375 to 0.09375
Outputs:
- logits: float32 [8192], P('dev')
The draws below stay inside these ranges and needn't reach their ends.
Inputs may be any that keep to these rules, and one draw needn't show every extreme that they name: `indices`: ids of rows of the table named by the second index.
All inputs are finite; a program needn't handle non-finite values.
Results may differ from the reference program's by a relative error of at most 0.0095.
Values may be sent and summed in bfloat16 or wider, within the bound.
A program may use at most 128 MiB of HBM per device.

```python
import jax
import jax.numpy as jnp
from jax import lax

E = 128
HID = 4096
TABLES = 32
POOL = 8
ROWS_DEV = 32768
RSPLIT = 4
ROWS = 131072
FEAT = 4096
BATCH = 8192


def plant(array, key, low, top_value):
    longest = array.shape.index(max(array.shape))
    spots = []
    for shift in (0, 1):
        where = [jax.random.randint(jax.random.fold_in(key, axis), (), 0, length) for axis, length in enumerate(array.shape)]
        where[longest] = (where[longest] + shift) % array.shape[longest]
        spots.append(tuple(where))
    return array.at[spots[0]].set(low).at[spots[1]].set(top_value)


def block_levels(key, shape, split, smallest, largest):
    level, own = 1.0, jax.random.fold_in(key, 6)
    for position, parts in split:
        draws = jnp.exp(jax.random.uniform(jax.random.fold_in(own, position), (parts,), jnp.float32, smallest / len(split), largest / len(split)))
        level = level * jnp.repeat(draws, shape[position] // parts).reshape([-1 if axis == position else 1 for axis in range(len(shape))])
    return level


def scatter_about(rng, dims, spread, limit, split=(), dtype=jnp.bfloat16):
    factor_of = block_levels(rng, dims, split, -0.22, 0.18) if split else 1.0
    values = jax.random.normal(rng, dims, jnp.float32) * spread * factor_of
    return jnp.minimum(jnp.maximum(values, -limit), limit).astype(dtype)


def setup_inputs(seed: int = 0) -> dict:
    arg_keys = jax.random.split(jax.random.key(seed), 7)
    indices = plant(jax.random.randint(arg_keys[0], (BATCH, TABLES, POOL), 0, ROWS), jax.random.fold_in(arg_keys[0], 1), 0, ROWS - 1).astype(jnp.int32)
    pool_len = plant(jax.random.randint(arg_keys[1], (TABLES,), 1, POOL + 1), jax.random.fold_in(arg_keys[1], 1), 1, POOL).astype(jnp.int32)
    tables = scatter_about(arg_keys[2], (TABLES * ROWS, E), 0.5, 3.0, ((0, 128),))
    w_first = scatter_about(arg_keys[3], (FEAT, HID), FEAT ** -0.5, 0.09375, ((0, 64), (1, 2)))
    b_first = scatter_about(arg_keys[4], (HID,), 0.5, 3.0, ((0, 2),))
    w_out = scatter_about(arg_keys[5], (HID,), HID ** -0.5, 0.09375, ((0, 2),))
    return {"indices": indices, "pool_len": pool_len, "tables": tables, "w_first": w_first, "b_first": b_first, "w_out": w_out}


def pool_table(inputs):
    table_rows, bag_ids, live_count = inputs
    gathered = jnp.take(table_rows, bag_ids, axis=0).astype(jnp.float32)
    slot_live = (jnp.arange(POOL) < live_count).astype(jnp.float32)
    row_block = bag_ids // ROWS_DEV
    owners = (row_block[:, :, None] == jnp.arange(RSPLIT)[None, None, :]).astype(jnp.float32)
    owners = owners * slot_live[None, :, None]
    partial_value = jnp.einsum('bpr,bpe->rbe', owners, gathered).astype(jnp.bfloat16)
    return jnp.sum(partial_value.astype(jnp.float32), axis=0).astype(jnp.bfloat16)


def reference(indices, pool_len, tables, w_first, b_first, w_out):
    table_view = tables.reshape(TABLES, ROWS, E)
    pooled = lax.map(pool_table, (table_view, jnp.transpose(indices, (1, 0, 2)), pool_len))
    flat_feat = jnp.transpose(pooled, (1, 0, 2)).reshape(BATCH, FEAT)
    pre_act = jnp.dot(flat_feat, w_first, preferred_element_type=jnp.float32) + b_first.astype(jnp.float32)
    hidden = jnp.maximum(pre_act, 0.0)
    return jnp.sum(hidden * w_out.astype(jnp.float32)[None, :], axis=1)
```

```python
import functools

import jax
import jax.numpy as jnp
from jax import lax
from jax.experimental import pallas as pl
from jax.experimental.pallas import tpu as pltpu
from jax.sharding import Mesh, PartitionSpec as P

TABLES = 32
SRC, BAGS, CAP = 128, 64, 512
CUTS = ((64, 32, 32), (16, 16, 16, 16, 32, 32), (32,) * 4)
G = 8
TB = 2048
NBUF = 4

def lookup_kernel(keys, table, out, rows_v, rows_s, tab, stage, buf, sem_s, sem_t):
    nb = table.shape[0] // TB
    def fetch(i, slot):
        return pltpu.make_async_copy(table.at[pl.ds(i * TB, TB), :], stage.at[slot], sem_t.at[slot])
    for i in range(NBUF):
        fetch(i, i).start()
    k = keys[...]
    n = jnp.sum((k < (BAGS << 15)).astype(jnp.int32), axis=1, keepdims=True)
    for r in range(4):
        rows_v[r * SRC:(r + 1) * SRC, :] = k[:, r * 128:(r + 1) * 128] & 32767
    rows_v[4 * SRC:, :] = jnp.broadcast_to(n, (SRC, 128))
    cps = [pltpu.make_async_copy(rows_v.at[pl.ds(i * SRC, SRC), :], rows_s.at[pl.ds(i * SRC, SRC), :], sem_s.at[i]) for i in range(5)]
    cps[4].start()
    cps[0].start()
    cps[1].start()
    buf[...] = jnp.zeros_like(buf)

    @pl.loop(0, nb // NBUF)
    def _(h):
        for slot in range(NBUF):
            i = h * NBUF + slot
            fetch(i, slot).wait()
            base = pl.multiple_of(i * TB, TB)
            tab[pl.ds(base, TB), :] = stage[slot].astype(jnp.float32)
            @pl.when(i + NBUF < nb)
            def _():
                fetch(i + NBUF, slot).start()

    cps[4].wait()
    cps[0].wait()
    cps[1].wait()
    most = lax.fori_loop(0, SRC, lambda c, m: jnp.maximum(m, rows_s[4 * SRC + c, 0]), 0, unroll=False)
    @pl.when(most > 256)
    def _():
        cps[2].start()
        cps[3].start()
        cps[2].wait()
        cps[3].wait()
    bag_row = lax.broadcasted_iota(jnp.int32, (BAGS, 256), 0)

    @pl.loop(0, SRC // G)
    def _(grp):
        @pl.loop(0, G)
        def _(g):
            c = grp * G + g
            n = rows_s[4 * SRC + c, 0]
            for r in range(4):
                def some(r=r):
                    view = rows_s.at[r * SRC + c]
                    at = 0
                    for size in CUTS[min(r, 2)]:
                        def block(at=at, size=size):
                            for u in range(at, at + size):
                                buf[g, r * 128 + u: r * 128 + u + 1, :] = tab[pl.ds(view[u], 1), :]
                        if at == 0:
                            block()
                        else:
                            pl.when(n > r * 128 + at)(block)
                        at += size
                if r == 0:
                    some()
                else:
                    pl.when(n > r * 128)(some)
        def part(g, lo):
            kk = keys[pl.ds(grp * G + g, 1), lo:lo + 256] >> 15
            oh = jnp.where(kk == bag_row, 1.0, 0.0).astype(jnp.bfloat16)
            return jnp.dot(oh, buf[g, lo:lo + 256, :].astype(jnp.bfloat16), preferred_element_type=jnp.float32)
        most = rows_s[4 * SRC + grp * G, 0]
        for g in range(1, G):
            most = jnp.maximum(most, rows_s[4 * SRC + grp * G + g, 0])
        for g in range(G):
            out[grp * G + g] = part(g, 0).astype(jnp.bfloat16)
        @pl.when(most > 256)
        def _():
            for g in range(G):
                out[grp * G + g] = (part(g, 0) + part(g, 256)).astype(jnp.bfloat16)


def lookup(keys, table):
    return pl.pallas_call(
        lookup_kernel,
        out_shape=jax.ShapeDtypeStruct((SRC, BAGS, 128), jnp.bfloat16),
        in_specs=[pl.BlockSpec(memory_space=pltpu.VMEM), pl.BlockSpec(memory_space=pl.ANY)],
        out_specs=pl.BlockSpec(memory_space=pltpu.VMEM),
        scratch_shapes=[
            pltpu.VMEM((SRC * 5, 128), jnp.int32),
            pltpu.SMEM((SRC * 5, 128), jnp.int32),
            pltpu.VMEM((table.shape[0], 128), jnp.float32),
            pltpu.VMEM((NBUF, TB, 128), jnp.bfloat16),
            pltpu.VMEM((G, CAP, 128), jnp.float32),
            pltpu.SemaphoreType.DMA((5,)),
            pltpu.SemaphoreType.DMA((NBUF,)),
        ],
        compiler_params=pltpu.CompilerParams(vmem_limit_bytes=48 << 20),
        cost_estimate=pl.CostEstimate(flops=10**10, bytes_accessed=10**7, transcendentals=0),
    )(keys, table)


LANES = 128
BLKS = CAP // LANES

def bitonic(xs, lane):
    pos = [lane + b * LANES for b in range(BLKS)]
    k = 2
    while k <= CAP:
        d = k // 2
        while d >= 1:
            if d >= LANES:
                step = d // LANES
                new = list(xs)
                for b in range(BLKS):
                    if b & step:
                        continue
                    lo, hi = jnp.minimum(xs[b], xs[b + step]), jnp.maximum(xs[b], xs[b + step])
                    up = ((b * LANES) & k) == 0
                    new[b], new[b + step] = (lo, hi) if up else (hi, lo)
                xs = new
            else:
                low = (lane & d) == 0
                new = []
                for b in range(BLKS):
                    x = xs[b]
                    other = jnp.where(low, pltpu.roll(x, LANES - d, 1), pltpu.roll(x, d, 1))
                    if k >= LANES:
                        up = ((b * LANES) & k) == 0
                        want_min = low if up else jnp.logical_not(low)
                    else:
                        want_min = ((pos[b] & k) == 0) == low
                    new.append(jnp.where(want_min, jnp.minimum(x, other), jnp.maximum(x, other)))
                xs = new
            d //= 2
        k *= 2
    return xs

def rotate_left(xs, lane, amount):
    s = 1
    while s < CAP:
        take = (amount & s) != 0
        if s >= LANES:
            step = s // LANES
            moved = [xs[(b + step) % BLKS] for b in range(BLKS)]
        else:
            rolled = [pltpu.roll(x, LANES - s, 1) for x in xs]
            moved = [jnp.where(lane < LANES - s, rolled[b], rolled[(b + 1) % BLKS]) for b in range(BLKS)]
        xs = [jnp.where(take, m, x) for m, x in zip(moved, xs)]
        s *= 2
    return xs

def prep_kernel(keys, out):
    lane = lax.broadcasted_iota(jnp.int32, (TABLES, LANES), 1)
    xs = bitonic([keys[:, b * LANES:(b + 1) * LANES] for b in range(BLKS)], lane)
    for j in range(4):
        ys = xs
        if j:
            start = sum(jnp.sum((x < (j << 21)).astype(jnp.int32), axis=1, keepdims=True) for x in xs)
            ys = rotate_left(xs, lane, jnp.broadcast_to(start, (TABLES, LANES)))
        for b in range(BLKS):
            mine = (ys[b] >> 21) == j
            out[j, :, b * LANES:(b + 1) * LANES] = jnp.where(mine, ys[b] & ((1 << 21) - 1), 64 << 15)


def prep(keys):
    return pl.pallas_call(
        prep_kernel,
        out_shape=jax.ShapeDtypeStruct((4, TABLES, CAP), jnp.int32),
        in_specs=[pl.BlockSpec(memory_space=pltpu.VMEM)],
        out_specs=pl.BlockSpec(memory_space=pltpu.VMEM),
    )(keys)


def make_keys(indices, pool_len):
    n, t, p = indices.shape
    bag = lax.broadcasted_iota(jnp.int32, (t, p, n), 2)
    slot = lax.broadcasted_iota(jnp.int32, (t, p, n), 1)
    idx = jnp.transpose(indices, (1, 2, 0))
    key = ((idx >> 15) << 21) | (bag << 15) | (idx & 32767)
    key = jnp.where(slot < pool_len[:, None, None], key, 4 << 21)
    return key.reshape(t, p * n)


ALL = ("section", "x", "z", "y")


def body(indices, pool_len, tables, w_first, b_first, w_out):
    x = lax.axis_index("x")
    z = lax.axis_index("z")
    y = lax.axis_index("y")
    quarter = w_first.shape[1] // 4
    w_part = lax.all_to_all(w_first, "x", split_axis=1, concat_axis=0, tiled=True)
    w_all = lax.all_gather(w_part.reshape(4, 64, quarter), ("z", "y"), axis=1)
    w_all = w_all.reshape(-1, quarter)
    bias = lax.dynamic_slice(b_first, (x * quarter,), (quarter,)).astype(jnp.float32)
    scale = lax.dynamic_slice(w_out, (x * quarter,), (quarter,)).astype(jnp.float32)

    lists = prep(make_keys(indices, pool_len))
    lists = jnp.transpose(lists, (1, 0, 2)).reshape(128, CAP)
    keys = lax.all_to_all(lists, ALL, split_axis=0, concat_axis=0, tiled=True)
    partial = lookup(keys, tables)
    ordered = jnp.transpose(partial.reshape(64, 2, BAGS, 128), (1, 0, 2, 3)).reshape(SRC, BAGS, 128)
    received = lax.all_to_all(ordered, ALL, split_axis=0, concat_axis=0, tiled=True)
    pooled = jnp.sum(received.reshape(TABLES, 4, BAGS, 128).astype(jnp.float32), axis=1)
    features = jnp.transpose(pooled.astype(jnp.bfloat16), (1, 0, 2)).reshape(BAGS, TABLES * 128)
    samples = lax.all_gather(features, ("x", "section"), axis=0, tiled=True)
    pre_act = jnp.dot(samples, w_all, preferred_element_type=jnp.float32)
    hidden = jnp.maximum(pre_act + bias[None, :], 0.0)
    logit_part = jnp.sum(hidden * scale[None, :], axis=1)
    parts = lax.all_gather(logit_part, ("section", "x"))
    total = jnp.sum(parts, axis=0)
    return lax.dynamic_slice(total, (x * 128,), (128,))


def solution(mesh):
    grid = Mesh(mesh.devices.reshape(2, 4, 4, 4), ALL)
    dev = ("x", "z", "y")
    placed = (
        P(ALL, None, None),
        P(),
        P(ALL, None),
        P(dev, "section"),
        P("section"),
        P("section"),
    )
    return jax.shard_map(body, mesh=grid, in_specs=placed, out_specs=P(dev), check_vma=False)
```

```python
import functools

import jax
import jax.numpy as jnp
from jax import lax
from jax.experimental import pallas as pl
from jax.experimental.pallas import tpu as pltpu
from jax.sharding import Mesh, PartitionSpec as P

TABLES = 32
SRC, BAGS, CAP = 128, 64, 512
CUTS = ((64, 32, 32), (16, 16, 16, 16, 32, 32), (32,) * 4)
G = 8
TB = 2048
NBUF = 4

def lookup_kernel(keys, table, out, rows_v, rows_s, tab, stage, buf, sem_s, sem_t):
    nb = table.shape[0] // TB
    def fetch(i, slot):
        return pltpu.make_async_copy(table.at[pl.ds(i * TB, TB), :], stage.at[slot], sem_t.at[slot])
    for i in range(NBUF):
        fetch(i, i).start()
    k = keys[...]
    n = jnp.sum((k < (BAGS << 15)).astype(jnp.int32), axis=1, keepdims=True)
    for r in range(4):
        rows_v[r * SRC:(r + 1) * SRC, :] = k[:, r * 128:(r + 1) * 128] & 32767
    rows_v[4 * SRC:, :] = jnp.broadcast_to(n, (SRC, 128))
    cps = [pltpu.make_async_copy(rows_v.at[pl.ds(i * SRC, SRC), :], rows_s.at[pl.ds(i * SRC, SRC), :], sem_s.at[i]) for i in range(5)]
    cps[4].start()
    cps[0].start()
    cps[1].start()
    buf[...] = jnp.zeros_like(buf)

    @pl.loop(0, nb // NBUF)
    def _(h):
        for slot in range(NBUF):
            i = h * NBUF + slot
            fetch(i, slot).wait()
            base = pl.multiple_of(i * TB, TB)
            tab[pl.ds(base, TB), :] = stage[slot].astype(jnp.float32)
            @pl.when(i + NBUF < nb)
            def _():
                fetch(i + NBUF, slot).start()

    cps[4].wait()
    cps[0].wait()
    cps[1].wait()
    most = lax.fori_loop(0, SRC, lambda c, m: jnp.maximum(m, rows_s[4 * SRC + c, 0]), 0, unroll=False)
    @pl.when(most > 256)
    def _():
        cps[2].start()
        cps[3].start()
        cps[2].wait()
        cps[3].wait()
    bag_row = lax.broadcasted_iota(jnp.int32, (BAGS, 256), 0)

    @pl.loop(0, SRC // G)
    def _(grp):
        @pl.loop(0, G)
        def _(g):
            c = grp * G + g
            n = rows_s[4 * SRC + c, 0]
            for r in range(4):
                def some(r=r):
                    view = rows_s.at[r * SRC + c]
                    at = 0
                    for size in CUTS[min(r, 2)]:
                        def block(at=at, size=size):
                            for u in range(at, at + size):
                                buf[g, r * 128 + u: r * 128 + u + 1, :] = tab[pl.ds(view[u], 1), :]
                        if at == 0:
                            block()
                        else:
                            pl.when(n > r * 128 + at)(block)
                        at += size
                if r == 0:
                    some()
                else:
                    pl.when(n > r * 128)(some)
        def part(g, lo):
            kk = keys[pl.ds(grp * G + g, 1), lo:lo + 256] >> 15
            oh = jnp.where(kk == bag_row, 1.0, 0.0).astype(jnp.bfloat16)
            return jnp.dot(oh, buf[g, lo:lo + 256, :].astype(jnp.bfloat16), preferred_element_type=jnp.float32)
        most = rows_s[4 * SRC + grp * G, 0]
        for g in range(1, G):
            most = jnp.maximum(most, rows_s[4 * SRC + grp * G + g, 0])
        for g in range(G):
            out[grp * G + g] = part(g, 0).astype(jnp.bfloat16)
        @pl.when(most > 256)
        def _():
            for g in range(G):
                out[grp * G + g] = (part(g, 0) + part(g, 256)).astype(jnp.bfloat16)


def lookup(keys, table):
    return pl.pallas_call(
        lookup_kernel,
        out_shape=jax.ShapeDtypeStruct((SRC, BAGS, 128), jnp.bfloat16),
        in_specs=[pl.BlockSpec(memory_space=pltpu.VMEM), pl.BlockSpec(memory_space=pl.ANY)],
        out_specs=pl.BlockSpec(memory_space=pltpu.VMEM),
        scratch_shapes=[
            pltpu.VMEM((SRC * 5, 128), jnp.int32),
            pltpu.SMEM((SRC * 5, 128), jnp.int32),
            pltpu.VMEM((table.shape[0], 128), jnp.float32),
            pltpu.VMEM((NBUF, TB, 128), jnp.bfloat16),
            pltpu.VMEM((G, CAP, 128), jnp.float32),
            pltpu.SemaphoreType.DMA((5,)),
            pltpu.SemaphoreType.DMA((NBUF,)),
        ],
        compiler_params=pltpu.CompilerParams(vmem_limit_bytes=48 << 20),
        cost_estimate=pl.CostEstimate(flops=10**10, bytes_accessed=10**7, transcendentals=0),
    )(keys, table)


LANES = 128
BLKS = CAP // LANES

def bitonic(xs, lane):
    pos = [lane + b * LANES for b in range(BLKS)]
    k = 2
    while k <= CAP:
        d = k // 2
        while d >= 1:
            if d >= LANES:
                step = d // LANES
                new = list(xs)
                for b in range(BLKS):
                    if b & step:
                        continue
                    lo, hi = jnp.minimum(xs[b], xs[b + step]), jnp.maximum(xs[b], xs[b + step])
                    up = ((b * LANES) & k) == 0
                    new[b], new[b + step] = (lo, hi) if up else (hi, lo)
                xs = new
            else:
                low = (lane & d) == 0
                new = []
                for b in range(BLKS):
                    x = xs[b]
                    other = jnp.where(low, pltpu.roll(x, LANES - d, 1), pltpu.roll(x, d, 1))
                    if k >= LANES:
                        up = ((b * LANES) & k) == 0
                        want_min = low if up else jnp.logical_not(low)
                    else:
                        want_min = ((pos[b] & k) == 0) == low
                    new.append(jnp.where(want_min, jnp.minimum(x, other), jnp.maximum(x, other)))
                xs = new
            d //= 2
        k *= 2
    return xs

def rotate_left(xs, lane, amount):
    s = 1
    while s < CAP:
        take = (amount & s) != 0
        if s >= LANES:
            step = s // LANES
            moved = [xs[(b + step) % BLKS] for b in range(BLKS)]
        else:
            rolled = [pltpu.roll(x, LANES - s, 1) for x in xs]
            moved = [jnp.where(lane < LANES - s, rolled[b], rolled[(b + 1) % BLKS]) for b in range(BLKS)]
        xs = [jnp.where(take, m, x) for m, x in zip(moved, xs)]
        s *= 2
    return xs

def prep_kernel(keys, out):
    lane = lax.broadcasted_iota(jnp.int32, (TABLES, LANES), 1)
    xs = bitonic([keys[:, b * LANES:(b + 1) * LANES] for b in range(BLKS)], lane)
    for j in range(4):
        ys = xs
        if j:
            start = sum(jnp.sum((x < (j << 21)).astype(jnp.int32), axis=1, keepdims=True) for x in xs)
            ys = rotate_left(xs, lane, jnp.broadcast_to(start, (TABLES, LANES)))
        for b in range(BLKS):
            mine = (ys[b] >> 21) == j
            out[j, :, b * LANES:(b + 1) * LANES] = jnp.where(mine, ys[b] & ((1 << 21) - 1), 64 << 15)


def prep(keys):
    return pl.pallas_call(
        prep_kernel,
        out_shape=jax.ShapeDtypeStruct((4, TABLES, CAP), jnp.int32),
        in_specs=[pl.BlockSpec(memory_space=pltpu.VMEM)],
        out_specs=pl.BlockSpec(memory_space=pltpu.VMEM),
    )(keys)


def make_keys(indices, pool_len):
    n, t, p = indices.shape
    bag = lax.broadcasted_iota(jnp.int32, (t, p, n), 2)
    slot = lax.broadcasted_iota(jnp.int32, (t, p, n), 1)
    idx = jnp.transpose(indices, (1, 2, 0))
    key = ((idx >> 15) << 21) | (bag << 15) | (idx & 32767)
    key = jnp.where(slot < pool_len[:, None, None], key, 4 << 21)
    return key.reshape(t, p * n)


MESH = pl.DeviceIdType.MESH
C = 4
(FAR_A, FAR_B, SUM_A, SUM_B, NEAR_A, NEAR_B, Z1, Z2, Z3, XR, XL, FWD_A, FWD_B, OWN_S, LEFT_S, RIGHT_S, FAR_SA, FAR_SB) = range(18)
KINDS = 18


def dense_kernel(part, w, bias, scale, out, mid_a, mid_b, from_l, from_r, pooled, feats, acc, plog, lrecv, ssem, rsem, lsend, lrec):
    s = lax.axis_index("section")
    x = lax.axis_index("x")
    z = lax.axis_index("z")
    y = lax.axis_index("y")
    right_y, left_y, far_y = lax.rem(y + 1, 4), lax.rem(y + 3, 4), lax.rem(y + 2, 4)
    right_x, left_x, far_x = lax.rem(x + 1, 4), lax.rem(x + 3, 4), lax.rem(x + 2, 4)
    other = 1 - s

    barrier = pltpu.get_barrier_semaphore()
    peers = [{"y": right_y}, {"y": left_y}]
    peers += [{"z": lax.rem(z + d, 4)} for d in (1, 2, 3)]
    peers += [{"x": lax.rem(x + d, 4)} for d in (1, 2, 3)]
    peers += [{"section": other}]
    peers += [{"section": other, "x": lax.rem(x + d, 4)} for d in (1, 2, 3)]
    for peer in peers:
        pl.semaphore_signal(barrier, inc=1, device_id=peer, device_id_type=MESH)
    pl.semaphore_wait(barrier, len(peers))

    def remote(src, dst, kind, c, peer):
        return pltpu.make_async_remote_copy(
            src_ref=src, dst_ref=dst, send_sem=ssem.at[kind, c], recv_sem=rsem.at[kind, c],
            device_id=peer, device_id_type=MESH,
        )

    A, B = pl.ds(0, 2), pl.ds(2, 2)
    copies = []
    for c in range(C):
        one = {
            FAR_A: remote(part.at[c, A, far_y], mid_a.at[c], FAR_A, c, {"y": right_y}),
            FAR_B: remote(part.at[c, B, far_y], mid_b.at[c], FAR_B, c, {"y": left_y}),
            SUM_A: remote(mid_a.at[c], from_l.at[c, A], SUM_A, c, {"y": right_y}),
            SUM_B: remote(mid_b.at[c], from_r.at[c, B], SUM_B, c, {"y": left_y}),
            NEAR_B: remote(part.at[c, B, right_y], from_l.at[c, B], NEAR_B, c, {"y": right_y}),
            NEAR_A: remote(part.at[c, A, left_y], from_r.at[c, A], NEAR_A, c, {"y": left_y}),
            XR: remote(feats.at[s, x, c], feats.at[s, x, c], XR, c, {"x": right_x}),
            XL: remote(feats.at[s, x, c], feats.at[s, x, c], XL, c, {"x": left_x}),
            FWD_A: remote(feats.at[s, left_x, c, A], feats.at[s, left_x, c, A], FWD_A, c, {"x": right_x}),
            FWD_B: remote(feats.at[s, right_x, c, B], feats.at[s, right_x, c, B], FWD_B, c, {"x": left_x}),
            OWN_S: remote(feats.at[s, x, c], feats.at[s, x, c], OWN_S, c, {"section": other}),
            LEFT_S: remote(feats.at[s, left_x, c], feats.at[s, left_x, c], LEFT_S, c, {"section": other}),
            RIGHT_S: remote(feats.at[s, right_x, c], feats.at[s, right_x, c], RIGHT_S, c, {"section": other}),
            FAR_SA: remote(feats.at[s, far_x, c, A], feats.at[s, far_x, c, A], FAR_SA, c, {"section": other}),
            FAR_SB: remote(feats.at[s, far_x, c, B], feats.at[s, far_x, c, B], FAR_SB, c, {"section": other}),
        }
        for i, kind in enumerate((Z1, Z2, Z3)):
            to = lax.rem(z + i + 1, 4)
            one[kind] = remote(pooled.at[c, to], feats.at[s, x, c, z], kind, c, {"z": to})
        copies.append(one)

    def start(c, *kinds):
        for kind in kinds:
            copies[c][kind].start()

    def arrive(c, *kinds):
        for kind in kinds:
            copies[c][kind].wait_recv()

    def stage_far(c):
        start(c, FAR_A, FAR_B)

    def stage_sum(c):
        arrive(c, FAR_A)
        mid_a[c] = (mid_a[c].astype(jnp.float32) + part[c, 0:2, right_y].astype(jnp.float32)).astype(jnp.bfloat16)
        start(c, SUM_A)
        arrive(c, FAR_B)
        mid_b[c] = (mid_b[c].astype(jnp.float32) + part[c, 2:4, left_y].astype(jnp.float32)).astype(jnp.bfloat16)
        start(c, SUM_B)
        start(c, NEAR_B, NEAR_A)
        if c + 2 < C:
            stage_far(c + 2)

    def stage_pool(c):
        arrive(c, SUM_A, NEAR_B, SUM_B, NEAR_A)
        total = part[c, :, y].astype(jnp.float32) + from_l[c].astype(jnp.float32) + from_r[c].astype(jnp.float32)
        pooled[c] = total.astype(jnp.bfloat16)
        start(c, Z1, Z3, Z2)
        feats[s, x, c, z] = pooled[c, z]

    def stage_x(c):
        arrive(c, Z1, Z3, Z2)
        start(c, XR, XL, OWN_S)

    def stage_fwd(c):
        arrive(c, XR)
        start(c, FWD_A, LEFT_S)
        arrive(c, XL)
        start(c, FWD_B, RIGHT_S)

    def stage_far_s(c):
        arrive(c, FWD_A)
        start(c, FAR_SA)
        arrive(c, FWD_B)
        start(c, FAR_SB)

    def stage_dense(c):
        arrive(c, OWN_S, LEFT_S, RIGHT_S, FAR_SA, FAR_SB)
        acc[...] = jnp.zeros_like(acc)

        @pl.loop(0, 8)
        def _(i):
            k0 = pl.multiple_of(i * 512, 512)
            si, xi = i // 4, lax.rem(i, 4)
            lhs = jnp.concatenate([feats[si, xi, c, j] for j in range(4)], axis=1)
            acc[...] += jnp.dot(lhs, w[pl.ds(k0, 512), :], preferred_element_type=jnp.float32)

        h = jnp.maximum(acc[...] + bias[...], 0.0) * scale[...]
        h = h[:, 0:128] + h[:, 128:256] + h[:, 256:384] + h[:, 384:512]
        plog[c] = jnp.sum(h.T, axis=0, keepdims=True)

    stage_far(0)
    stage_far(1)
    stages = (stage_sum, stage_pool, stage_x, stage_fwd, stage_far_s, stage_dense)
    for step in range(C + len(stages) - 1):
        for i, stage in enumerate(stages):
            if 0 <= step - i < C:
                stage(step - i)

    sent = []
    for ds in range(2):
        for dx in range(4):
            if ds == 0 and dx == 0:
                continue
            to_s = s if ds == 0 else other
            to_x = lax.rem(x + dx, 4)
            k = ds * 4 + dx
            copy = pltpu.make_async_remote_copy(
                src_ref=plog.at[to_x], dst_ref=lrecv.at[s * 4 + x], send_sem=lsend.at[k], recv_sem=lrec.at[k],
                device_id={"section": to_s, "x": to_x}, device_id_type=MESH,
            )
            copy.start()
            sent.append(copy)
    lrecv[s * 4 + x] = plog[x]
    for copy in sent:
        copy.wait_recv()
    total = lrecv[0]
    for i in range(1, 8):
        total = total + lrecv[i]
    out[...] = total
    for copy in sent:
        copy.wait_send()
    for c in range(C):
        for kind in range(KINDS):
            copies[c][kind].wait_send()


def dense(partial, w, bias, scale):
    bf = jnp.bfloat16
    vmem = pl.BlockSpec(memory_space=pltpu.VMEM)
    return pl.pallas_call(
        dense_kernel,
        out_shape=jax.ShapeDtypeStruct((1, 128), jnp.float32),
        in_specs=[vmem] * 4,
        out_specs=vmem,
        scratch_shapes=[
            pltpu.VMEM((C, 2, 128, 128), bf),
            pltpu.VMEM((C, 2, 128, 128), bf),
            pltpu.VMEM((C, 4, 128, 128), bf),
            pltpu.VMEM((C, 4, 128, 128), bf),
            pltpu.VMEM((C, 4, 128, 128), bf),
            pltpu.VMEM((2, 4, C, 4, 128, 128), bf),
            pltpu.VMEM((128, 512), jnp.float32),
            pltpu.VMEM((C, 1, 128), jnp.float32),
            pltpu.VMEM((8, 1, 128), jnp.float32),
            pltpu.SemaphoreType.DMA((KINDS, C)),
            pltpu.SemaphoreType.DMA((KINDS, C)),
            pltpu.SemaphoreType.DMA((8,)),
            pltpu.SemaphoreType.DMA((8,)),
        ],
        compiler_params=pltpu.CompilerParams(collective_id=1, has_side_effects=True, vmem_limit_bytes=48 << 20),
        cost_estimate=pl.CostEstimate(flops=3 * 10**10, bytes_accessed=10**7, transcendentals=0),
    )(partial.reshape(4, 4, 4, 128, 128), w, bias, scale)


ALL = ("section", "x", "z", "y")


def body(indices, pool_len, tables, w_first, b_first, w_out):
    x = lax.axis_index("x")
    z = lax.axis_index("z")
    y = lax.axis_index("y")
    quarter = w_first.shape[1] // 4
    w_part = lax.all_to_all(w_first, "x", split_axis=1, concat_axis=0, tiled=True)
    w_all = lax.all_gather(w_part.reshape(4, 64, quarter), ("z", "y"), axis=1)
    w_all = w_all.reshape(-1, quarter)
    bias = lax.dynamic_slice(b_first, (x * quarter,), (quarter,)).astype(jnp.float32)
    scale = lax.dynamic_slice(w_out, (x * quarter,), (quarter,)).astype(jnp.float32)

    lists = prep(make_keys(indices, pool_len))
    lists = jnp.transpose(lists, (1, 0, 2)).reshape(128, CAP)
    keys = lax.all_to_all(lists, ALL, split_axis=0, concat_axis=0, tiled=True)
    partial = lookup(keys, tables)
    return dense(partial, w_all, bias[None, :], scale[None, :]).reshape(128)


def solution(mesh):
    grid = Mesh(mesh.devices.reshape(2, 4, 4, 4), ALL)
    dev = ("x", "z", "y")
    placed = (
        P(ALL, None, None),
        P(),
        P(ALL, None),
        P(dev, "section"),
        P("section"),
        P("section"),
    )
    return jax.shard_map(body, mesh=grid, in_specs=placed, out_specs=P(dev), check_vma=False)
```

```python
import functools

import jax
import jax.numpy as jnp
from jax import lax
from jax.experimental import pallas as pl
from jax.experimental.pallas import tpu as pltpu
from jax.sharding import Mesh, PartitionSpec as P

TABLES = 32
SRC, BAGS, CAP = 128, 64, 512
TAIL = (16, 16, 16, 16, 32, 32)
G = 8
TB = 2048
NBUF = 4


def lookup_kernel(lists, tab, out, keys, rows_v, n_v, rows_s, n_s, buf, sem_n, sem_r, sem_f):
    y = lax.axis_index("y")
    lane = lax.broadcasted_iota(jnp.int32, (SRC, LANES), 1)
    blocks = [lists[:, b * LANES:(b + 1) * LANES] for b in range(BLKS)]
    first = sum(jnp.sum((v < (y << 21)).astype(jnp.int32), axis=1, keepdims=True) for v in blocks)
    blocks = rotate_left(blocks, lane, jnp.broadcast_to(first, (SRC, LANES)))
    n = jnp.zeros((SRC, 1), jnp.int32)
    for b in range(BLKS):
        mine = (blocks[b] >> 21) == y
        n += jnp.sum(mine.astype(jnp.int32), axis=1, keepdims=True)
        keys[:, b * LANES:(b + 1) * LANES] = jnp.where(mine, (blocks[b] >> 15) & 63, BAGS)
        rows_v[b] = jnp.where(mine, blocks[b] & 32767, 0)
    n_v[...] = jnp.broadcast_to(n, (SRC, LANES)).T[0:8]
    n_copy = pltpu.make_async_copy(n_v, n_s, sem_n)
    n_copy.start()

    def tile(r, grp, slot, sem):
        rows = pl.ds(pl.multiple_of(grp * G, G), G)
        return pltpu.make_async_copy(rows_v.at[r, rows, :], rows_s.at[slot, r], sem)

    for r in range(2):
        tile(r, 0, 0, sem_r.at[0, r]).start()
    buf[...] = jnp.zeros_like(buf)
    n_copy.wait()

    bag_row = lax.broadcasted_iota(jnp.int32, (BAGS, 256), 0)

    def part(grp, slot, g, lo):
        kk = keys[pl.ds(grp * G + g, 1), lo:lo + 256]
        oh = jnp.where(kk == bag_row, 1.0, 0.0).astype(jnp.bfloat16)
        return jnp.dot(oh, buf[slot, g, lo:lo + 256, :].astype(jnp.bfloat16), preferred_element_type=jnp.float32)

    def place(grp, g):
        return ((grp >> 1) & 1) * 64 + (grp & 1) * 8 + (grp >> 2) + (g % 4) * 16 + (g // 4) * 4

    def pool(grp, slot):
        for g in range(G):
            out[place(grp, g)] = part(grp, slot, g, 0).astype(jnp.bfloat16)

    def long_lists(grp, slot):
        most = n_s[0, grp * G]
        for g in range(1, G):
            most = jnp.maximum(most, n_s[0, grp * G + g])

        @pl.when(most > 256)
        def _():
            for r in (2, 3):
                copy = tile(r, grp, slot, sem_f)
                copy.start()
                copy.wait()

            for g in range(G):
                for r in (2, 3):
                    @pl.loop(0, 128)
                    def _(u):
                        buf[slot, g, pl.ds(r * 128 + u, 1), :] = tab[pl.ds(rows_s[slot, r, g, u], 1), :]
                total = part(grp, slot, g, 0) + part(grp, slot, g, 256)
                out[place(grp, g)] = total.astype(jnp.bfloat16)

    @pl.loop(0, SRC // G // 2)
    def _(h):
        for slot in range(2):
            grp = h * 2 + slot
            for r in range(2):
                tile(r, grp, slot, sem_r.at[slot, r]).wait()

            @pl.when(grp + 1 < SRC // G)
            def _():
                for r in range(2):
                    tile(r, grp + 1, 1 - slot, sem_r.at[1 - slot, r]).start()

            before = jnp.maximum(grp - 1, 0)
            for g in range(G):
                for u in range(128):
                    buf[slot, g, u:u + 1, :] = tab[pl.ds(rows_s[slot, 0, g, u], 1), :]
            pool(before, 1 - slot)
            for g in range(G):
                count = n_s[0, grp * G + g]
                at = 0
                for size in TAIL:
                    @pl.when(count > 128 + at)
                    def _(at=at, size=size):
                        for u in range(at, at + size):
                            buf[slot, g, 128 + u:129 + u, :] = tab[pl.ds(rows_s[slot, 1, g, u], 1), :]
                    at += size
            long_lists(before, 1 - slot)

    pool(SRC // G - 1, 1)
    long_lists(SRC // G - 1, 1)


def lookup(lists, tab):
    vmem = pl.BlockSpec(memory_space=pltpu.VMEM)
    return pl.pallas_call(
        lookup_kernel,
        out_shape=pltpu.VMEM((SRC, BAGS, 128), jnp.bfloat16),
        in_specs=[vmem, vmem],
        out_specs=vmem,
        scratch_shapes=[
            pltpu.VMEM((SRC, CAP), jnp.int32),
            pltpu.VMEM((4, SRC, 128), jnp.int32),
            pltpu.VMEM((8, 128), jnp.int32),
            pltpu.SMEM((2, 4, G, 128), jnp.int32),
            pltpu.SMEM((8, 128), jnp.int32),
            pltpu.VMEM((2, G, CAP, 128), jnp.float32),
            pltpu.SemaphoreType.DMA,
            pltpu.SemaphoreType.DMA((2, 2)),
            pltpu.SemaphoreType.DMA,
        ],
        compiler_params=pltpu.CompilerParams(vmem_limit_bytes=32 << 20),
        cost_estimate=pl.CostEstimate(flops=10**10, bytes_accessed=10**7, transcendentals=0),
    )(lists, tab)


LANES = 128
BLKS = CAP // LANES

def bitonic(xs, lane):
    pos = [lane + b * LANES for b in range(BLKS)]
    k = 2
    while k <= CAP:
        d = k // 2
        while d >= 1:
            if d >= LANES:
                step = d // LANES
                new = list(xs)
                for b in range(BLKS):
                    if b & step:
                        continue
                    lo, hi = jnp.minimum(xs[b], xs[b + step]), jnp.maximum(xs[b], xs[b + step])
                    up = ((b * LANES) & k) == 0
                    new[b], new[b + step] = (lo, hi) if up else (hi, lo)
                xs = new
            else:
                low = (lane & d) == 0
                new = []
                for b in range(BLKS):
                    x = xs[b]
                    other = jnp.where(low, pltpu.roll(x, LANES - d, 1), pltpu.roll(x, d, 1))
                    if k >= LANES:
                        up = ((b * LANES) & k) == 0
                        want_min = low if up else jnp.logical_not(low)
                    else:
                        want_min = ((pos[b] & k) == 0) == low
                    new.append(jnp.where(want_min, jnp.minimum(x, other), jnp.maximum(x, other)))
                xs = new
            d //= 2
        k *= 2
    return xs

def rotate_left(xs, lane, amount):
    s = 1
    while s < CAP:
        take = (amount & s) != 0
        if s >= LANES:
            step = s // LANES
            moved = [xs[(b + step) % BLKS] for b in range(BLKS)]
        else:
            rolled = [pltpu.roll(x, LANES - s, 1) for x in xs]
            moved = [jnp.where(lane < LANES - s, rolled[b], rolled[(b + 1) % BLKS]) for b in range(BLKS)]
        xs = [jnp.where(take, m, x) for m, x in zip(moved, xs)]
        s *= 2
    return xs

WZR, WZL, WYR, WYL, WFZR, WFZL, WFYR, WFYL = range(8)


def front_kernel(keys, w, table, lists, w_a, w_b, tab, own, from_x, to_z, from_z, both, stage, xs, xr, ls, lr, gs, gr, sem_t):
    s = lax.axis_index("section")
    x = lax.axis_index("x")
    z = lax.axis_index("z")
    y = lax.axis_index("y")
    other = 1 - s
    nb = table.shape[0] // TB

    def fetch(i, slot):
        return pltpu.make_async_copy(table.at[pl.ds(i * TB, TB), :], stage.at[slot], sem_t.at[slot])

    for i in range(NBUF):
        fetch(i, i).start()

    def widen(h):
        @pl.loop(h * (nb // NBUF) // 4, (h + 1) * (nb // NBUF) // 4)
        def _(k):
            for slot in range(NBUF):
                i = k * NBUF + slot
                fetch(i, slot).wait()
                tab[pl.ds(pl.multiple_of(i * TB, TB), TB), :] = stage[slot].astype(jnp.float32)

                @pl.when(i + NBUF < nb)
                def _():
                    fetch(i + NBUF, slot).start()

    barrier = pltpu.get_barrier_semaphore()
    peers = [{"section": other}]
    for axis, at in (("x", x), ("z", z), ("y", y)):
        peers += [{axis: lax.rem(at + d, 4)} for d in (1, 2, 3)]
    for peer in peers:
        pl.semaphore_signal(barrier, inc=1, device_id=peer, device_id_type=MESH)

    lane = lax.broadcasted_iota(jnp.int32, (TABLES, LANES), 1)
    blocks = bitonic([keys[:, b * LANES:(b + 1) * LANES] for b in range(BLKS)], lane)
    for b in range(BLKS):
        own[:, :, b * LANES:(b + 1) * LANES] = blocks[b].reshape(4, 8, LANES)
    pl.semaphore_wait(barrier, len(peers))

    def list_copy(k, src, dst, peer):
        return pltpu.make_async_remote_copy(
            src_ref=src, dst_ref=dst, send_sem=ls.at[k], recv_sem=lr.at[k], device_id=peer, device_id_type=MESH,
        )

    sent = []
    along_x = []
    for i in range(3):
        to = lax.rem(x + i + 1, 4)
        along_x.append(list_copy(i, own.at[to], from_x.at[x], {"x": to}))
    for copy in along_x:
        copy.start()

    x_copies = []
    for i in range(3):
        to = lax.rem(x + i + 1, 4)
        for half, full, mine in ((0, w_a, z), (1, w_b, y)):
            cols = pl.ds(pl.multiple_of(to * 512 + half * 256, 256), 256)
            copy = pltpu.make_async_remote_copy(
                src_ref=w.at[:, cols], dst_ref=full.at[mine, x], send_sem=xs.at[i, half], recv_sem=xr.at[i, half],
                device_id={"x": to}, device_id_type=MESH,
            )
            copy.start()
            x_copies.append(copy)
    for half, full, mine in ((0, w_a, z), (1, w_b, y)):
        cols = pl.ds(pl.multiple_of(x * 512 + half * 256, 256), 256)
        full[mine, x] = w[:, cols]
    from_x[x] = own[x]
    widen(0)

    def ring(kind, ref, axis, to):
        return pltpu.make_async_remote_copy(
            src_ref=ref, dst_ref=ref, send_sem=gs.at[kind], recv_sem=gr.at[kind], device_id={axis: to}, device_id_type=MESH,
        )

    z_right, z_left = lax.rem(z + 1, 4), lax.rem(z + 3, 4)
    y_right, y_left = lax.rem(y + 1, 4), lax.rem(y + 3, 4)
    low, high = pl.ds(0, 2), pl.ds(2, 2)
    near = [
        ring(WZR, w_a.at[z], "z", z_right), ring(WZL, w_a.at[z], "z", z_left),
        ring(WYR, w_b.at[y], "y", y_right), ring(WYL, w_b.at[y], "y", y_left),
    ]
    far = [
        ring(WFZR, w_a.at[z_left, low], "z", z_right), ring(WFZL, w_a.at[z_right, high], "z", z_left),
        ring(WFYR, w_b.at[y_left, low], "y", y_right), ring(WFYL, w_b.at[y_right, high], "y", y_left),
    ]
    for copy in along_x:
        copy.wait_recv()
    for xi in range(4):
        for si in range(2):
            for zi in range(4):
                to_z[zi, si * 4 + xi:si * 4 + xi + 1, :] = from_x[xi, si * 4 + zi:si * 4 + zi + 1, :]
    along_z = []
    for i in range(3):
        to = lax.rem(z + i + 1, 4)
        along_z.append(list_copy(3 + i, to_z.at[to], from_z.at[z], {"z": to}))
    for copy in along_z:
        copy.start()
    from_z[z] = to_z[z]
    for copy in x_copies:
        copy.wait_recv()
    for copy in near:
        copy.start()
    widen(1)

    for copy in along_z:
        copy.wait_recv()
    for zi in range(4):
        for si in range(2):
            both[si, zi * 4:zi * 4 + 4, :] = from_z[zi, si * 4:si * 4 + 4, :]
    across = list_copy(6, both.at[other], lists.at[y, s], {"section": other})
    across.start()
    along_y = []
    for i in range(3):
        along_y.append(list_copy(7 + i, both.at[s], lists.at[y, s], {"y": lax.rem(y + i + 1, 4)}))
    for copy in along_y:
        copy.start()
    lists[y, s] = both[s]
    across.wait_recv()
    for i in range(3):
        copy = list_copy(10 + i, lists.at[y, other], lists.at[y, other], {"y": lax.rem(y + i + 1, 4)})
        copy.start()
        along_y.append(copy)

    widen(2)
    for copy, onward in zip(near, far):
        copy.wait_recv()
        onward.start()
    widen(3)
    for copy in along_y + far:
        copy.wait_recv()
    for copy in along_x + along_z + [across] + along_y + x_copies + near + far:
        copy.wait_send()


def front(keys, w, table):
    vmem = pl.BlockSpec(memory_space=pltpu.VMEM)
    piece = pltpu.VMEM((4, 4, 64, 256), jnp.bfloat16)
    rows = pltpu.VMEM((4, 8, CAP), jnp.int32)
    dma = pltpu.SemaphoreType.DMA
    return pl.pallas_call(
        front_kernel,
        out_shape=(
            pltpu.VMEM((4, 2, 16, CAP), jnp.int32), piece, piece, pltpu.VMEM(table.shape, jnp.float32),
        ),
        in_specs=[vmem, vmem, pl.BlockSpec(memory_space=pl.ANY)],
        out_specs=(vmem,) * 4,
        scratch_shapes=[
            rows, rows, rows, rows,
            pltpu.VMEM((2, 16, CAP), jnp.int32),
            pltpu.VMEM((NBUF, TB, 128), jnp.bfloat16),
            dma((3, 2)), dma((3, 2)), dma((13,)), dma((13,)), dma((8,)), dma((8,)), dma((NBUF,)),
        ],
        compiler_params=pltpu.CompilerParams(collective_id=0, has_side_effects=True, vmem_limit_bytes=40 << 20),
        cost_estimate=pl.CostEstimate(flops=10**10, bytes_accessed=10**7, transcendentals=0),
    )(keys, w, table)


def make_keys(indices, pool_len):
    n, t, p = indices.shape
    bag = lax.broadcasted_iota(jnp.int32, (t, p, n), 2)
    slot = lax.broadcasted_iota(jnp.int32, (t, p, n), 1)
    idx = jnp.transpose(indices, (1, 2, 0))
    key = ((idx >> 15) << 21) | (bag << 15) | (idx & 32767)
    key = jnp.where(slot < pool_len[:, None, None], key, 4 << 21)
    return jnp.transpose(key.reshape(2, 4, 4, p * n), (1, 0, 2, 3)).reshape(t, p * n)


MESH = pl.DeviceIdType.MESH
C = 4
(FAR_A, FAR_B, SUM_A, SUM_B, NEAR_A, NEAR_B, Z1, Z2, Z3, XR, XL, FWD_A, FWD_B, OWN_S, LEFT_S, RIGHT_S, FAR_SA, FAR_SB) = range(18)
KINDS = 18


def dense_kernel(part, w_a, w_b, bias, scale, out, mid_a, mid_b, from_l, from_r, pooled, feats, acc, plog, lrecv, full_a, full_b, ssem, rsem, lsend, lrec, wsend, wrecv):
    s = lax.axis_index("section")
    x = lax.axis_index("x")
    z = lax.axis_index("z")
    y = lax.axis_index("y")
    right_y, left_y, far_y = lax.rem(y + 1, 4), lax.rem(y + 3, 4), lax.rem(y + 2, 4)
    right_x, left_x, far_x = lax.rem(x + 1, 4), lax.rem(x + 3, 4), lax.rem(x + 2, 4)
    other = 1 - s

    barrier = pltpu.get_barrier_semaphore()
    peers = [{"y": right_y}, {"y": left_y}]
    peers += [{"z": lax.rem(z + d, 4)} for d in (1, 2, 3)]
    peers += [{"x": lax.rem(x + d, 4)} for d in (1, 2, 3)]
    peers += [{"section": other}]
    peers += [{"section": other, "x": lax.rem(x + d, 4)} for d in (1, 2, 3)]
    for peer in peers:
        pl.semaphore_signal(barrier, inc=1, device_id=peer, device_id_type=MESH)
    pl.semaphore_wait(barrier, len(peers))

    def remote(src, dst, kind, c, peer):
        return pltpu.make_async_remote_copy(
            src_ref=src, dst_ref=dst, send_sem=ssem.at[kind, c], recv_sem=rsem.at[kind, c],
            device_id=peer, device_id_type=MESH,
        )

    A, B = pl.ds(0, 2), pl.ds(2, 2)
    copies = []
    for c in range(C):
        one = {
            FAR_A: remote(part.at[c, A, far_y], mid_a.at[c], FAR_A, c, {"y": right_y}),
            FAR_B: remote(part.at[c, B, far_y], mid_b.at[c], FAR_B, c, {"y": left_y}),
            SUM_A: remote(mid_a.at[c], from_l.at[c, A], SUM_A, c, {"y": right_y}),
            SUM_B: remote(mid_b.at[c], from_r.at[c, B], SUM_B, c, {"y": left_y}),
            NEAR_B: remote(part.at[c, B, right_y], from_l.at[c, B], NEAR_B, c, {"y": right_y}),
            NEAR_A: remote(part.at[c, A, left_y], from_r.at[c, A], NEAR_A, c, {"y": left_y}),
            XR: remote(feats.at[s, x, c], feats.at[s, x, c], XR, c, {"x": right_x}),
            XL: remote(feats.at[s, x, c], feats.at[s, x, c], XL, c, {"x": left_x}),
            FWD_A: remote(feats.at[s, left_x, c, A], feats.at[s, left_x, c, A], FWD_A, c, {"x": right_x}),
            FWD_B: remote(feats.at[s, right_x, c, B], feats.at[s, right_x, c, B], FWD_B, c, {"x": left_x}),
            OWN_S: remote(feats.at[s, x, c], feats.at[s, x, c], OWN_S, c, {"section": other}),
            LEFT_S: remote(feats.at[s, left_x, c], feats.at[s, left_x, c], LEFT_S, c, {"section": other}),
            RIGHT_S: remote(feats.at[s, right_x, c], feats.at[s, right_x, c], RIGHT_S, c, {"section": other}),
            FAR_SA: remote(feats.at[s, far_x, c, A], feats.at[s, far_x, c, A], FAR_SA, c, {"section": other}),
            FAR_SB: remote(feats.at[s, far_x, c, B], feats.at[s, far_x, c, B], FAR_SB, c, {"section": other}),
        }
        for i, kind in enumerate((Z1, Z2, Z3)):
            to = lax.rem(z + i + 1, 4)
            one[kind] = remote(pooled.at[c, to], feats.at[s, x, c, z], kind, c, {"z": to})
        copies.append(one)

    def start(c, *kinds):
        for kind in kinds:
            copies[c][kind].start()

    def arrive(c, *kinds):
        for kind in kinds:
            copies[c][kind].wait_recv()

    right_z, left_z, far_z = lax.rem(z + 1, 4), lax.rem(z + 3, 4), lax.rem(z + 2, 4)

    def w_copy(k, i, src, full, row, axis, to):
        return pltpu.make_async_remote_copy(
            src_ref=src.at[i] if src is not full else full.at[row, i], dst_ref=full.at[row, i],
            send_sem=wsend.at[k, i], recv_sem=wrecv.at[k, i], device_id={axis: to}, device_id_type=MESH,
        )

    w_near, w_far = {}, {}
    for half, (src, full, axis, mine, right, left) in enumerate(
        ((w_a, full_a, "y", y, right_y, left_y), (w_b, full_b, "z", z, right_z, left_z))
    ):
        for i in range(4):
            w_near[half, 0, i] = w_copy(half * 4, i, src, full, mine, axis, right)
            w_near[half, 1, i] = w_copy(half * 4 + 1, i, src, full, mine, axis, left)
        for i in range(2):
            w_far[half, 0, i] = w_copy(half * 4 + 2, i, full, full, left, axis, right)
            w_far[half, 1, i] = w_copy(half * 4 + 3, i + 2, full, full, right, axis, left)

    def w_start(half, *pieces):
        for i in pieces:
            w_near[half, 0, i].start()
            w_near[half, 1, i].start()

    def w_onward(half, i):
        w_near[half, 0, i].wait_recv()
        w_far[half, 0, i].start()
        w_near[half, 1, i + 2].wait_recv()
        w_far[half, 1, i].start()

    def w_arrive():
        for half in range(2):
            for i in range(2):
                w_near[half, 0, i + 2].wait_recv()
                w_near[half, 1, i].wait_recv()
                w_far[half, 0, i].wait_recv()
                w_far[half, 1, i].wait_recv()

    def stage_far(c):
        start(c, FAR_A, FAR_B)

    def stage_sum(c):
        arrive(c, FAR_A)
        mid_a[c] = (mid_a[c].astype(jnp.float32) + part[c, 0:2, right_y].astype(jnp.float32)).astype(jnp.bfloat16)
        start(c, SUM_A)
        arrive(c, FAR_B)
        mid_b[c] = (mid_b[c].astype(jnp.float32) + part[c, 2:4, left_y].astype(jnp.float32)).astype(jnp.bfloat16)
        start(c, SUM_B)
        start(c, NEAR_B, NEAR_A)
        if c + 2 < C:
            stage_far(c + 2)

    def stage_pool(c):
        arrive(c, SUM_A, NEAR_B, SUM_B, NEAR_A)
        total = part[c, :, y].astype(jnp.float32) + from_l[c].astype(jnp.float32) + from_r[c].astype(jnp.float32)
        pooled[c] = total.astype(jnp.bfloat16)
        start(c, Z1, Z3, Z2)
        feats[s, x, c, z] = pooled[c, z]

    def stage_x(c):
        arrive(c, Z1, Z3, Z2)
        start(c, XR, XL, OWN_S)

    def stage_fwd(c):
        arrive(c, XR)
        start(c, FWD_A, LEFT_S)
        arrive(c, XL)
        start(c, FWD_B, RIGHT_S)

    def stage_far_s(c):
        arrive(c, FWD_A)
        start(c, FAR_SA)
        arrive(c, FWD_B)
        start(c, FAR_SB)

    def dense_rows(first, last):
        rows = (last - first) * 128
        for c in range(first, last):
            arrive(c, OWN_S, LEFT_S, RIGHT_S, FAR_SA, FAR_SB)
        acc[0:rows] = jnp.zeros((rows, 512), jnp.float32)

        @pl.loop(0, 8)
        def _(i):
            si, xi = i // 4, lax.rem(i, 4)
            zi, wx = 2 * lax.rem(i, 2), i // 2
            lhs = jnp.concatenate(
                [jnp.concatenate([feats[si, xi, c, j] for j in range(4)], axis=1) for c in range(first, last)], axis=0
            )
            rhs_a = jnp.concatenate([full_a[yy, zi + zz, wx] for zz in range(2) for yy in range(4)], axis=0)
            acc[0:rows, 0:256] += jnp.dot(lhs, rhs_a, preferred_element_type=jnp.float32)
            rhs_b = jnp.concatenate([full_b[zi + zz, yy, wx] for zz in range(2) for yy in range(4)], axis=0)
            acc[0:rows, 256:512] += jnp.dot(lhs, rhs_b, preferred_element_type=jnp.float32)

        for k in range(rows // 128):
            h = jnp.maximum(acc[k * 128:(k + 1) * 128] + bias[...], 0.0) * scale[...]
            h = h[:, 0:128] + h[:, 128:256] + h[:, 256:384] + h[:, 384:512]
            plog[first + k] = jnp.sum(h.T, axis=0, keepdims=True)

    stage_far(0)
    stage_far(1)
    w_start(1, 0, 2)
    full_a[y] = w_a[...]
    full_b[z] = w_b[...]
    stages = (stage_sum, stage_pool, stage_x, stage_fwd, stage_far_s)
    for step in range(C + len(stages) - 1):
        if step == C + 3:
            w_arrive()
            dense_rows(0, 3)
        for i, stage in enumerate(stages):
            if 0 <= step - i < C:
                stage(step - i)
        if step == 1:
            w_start(1, 1, 3)
        elif step == 2:
            w_onward(1, 0)
        elif step == 3:
            w_onward(1, 1)
            w_start(0, 0, 2, 1, 3)
        elif step == 5:
            w_onward(0, 0)
        elif step == 6:
            w_onward(0, 1)
    dense_rows(3, 4)

    sent = []
    for ds in range(2):
        for dx in range(4):
            if ds == 0 and dx == 0:
                continue
            to_s = s if ds == 0 else other
            to_x = lax.rem(x + dx, 4)
            k = ds * 4 + dx
            copy = pltpu.make_async_remote_copy(
                src_ref=plog.at[to_x], dst_ref=lrecv.at[s * 4 + x], send_sem=lsend.at[k], recv_sem=lrec.at[k],
                device_id={"section": to_s, "x": to_x}, device_id_type=MESH,
            )
            copy.start()
            sent.append(copy)
    lrecv[s * 4 + x] = plog[x]
    for copy in sent:
        copy.wait_recv()
    total = lrecv[0]
    for i in range(1, 8):
        total = total + lrecv[i]
    out[...] = total
    for copy in sent + list(w_near.values()) + list(w_far.values()):
        copy.wait_send()
    for c in range(C):
        for kind in range(KINDS):
            copies[c][kind].wait_send()


def dense(partial, w_a, w_b, bias, scale):
    bf = jnp.bfloat16
    vmem = pl.BlockSpec(memory_space=pltpu.VMEM)
    return pl.pallas_call(
        dense_kernel,
        out_shape=jax.ShapeDtypeStruct((1, 128), jnp.float32),
        in_specs=[vmem] * 5,
        out_specs=vmem,
        scratch_shapes=[
            pltpu.VMEM((C, 2, 128, 128), bf),
            pltpu.VMEM((C, 2, 128, 128), bf),
            pltpu.VMEM((C, 4, 128, 128), bf),
            pltpu.VMEM((C, 4, 128, 128), bf),
            pltpu.VMEM((C, 4, 128, 128), bf),
            pltpu.VMEM((2, 4, C, 4, 128, 128), bf),
            pltpu.VMEM((384, 512), jnp.float32),
            pltpu.VMEM((C, 1, 128), jnp.float32),
            pltpu.VMEM((8, 1, 128), jnp.float32),
            pltpu.VMEM((4, 4, 4, 64, 256), bf),
            pltpu.VMEM((4, 4, 4, 64, 256), bf),
            pltpu.SemaphoreType.DMA((KINDS, C)),
            pltpu.SemaphoreType.DMA((KINDS, C)),
            pltpu.SemaphoreType.DMA((8,)),
            pltpu.SemaphoreType.DMA((8,)),
            pltpu.SemaphoreType.DMA((8, 4)),
            pltpu.SemaphoreType.DMA((8, 4)),
        ],
        compiler_params=pltpu.CompilerParams(collective_id=1, has_side_effects=True, vmem_limit_bytes=48 << 20),
        cost_estimate=pl.CostEstimate(flops=3 * 10**10, bytes_accessed=10**7, transcendentals=0),
    )(partial.reshape(4, 4, 4, 128, 128), w_a, w_b, bias, scale)


ALL = ("section", "x", "z", "y")


def body(indices, pool_len, tables, w_first, b_first, w_out):
    x = lax.axis_index("x")
    quarter = w_first.shape[1] // 4
    bias = lax.dynamic_slice(b_first, (x * quarter,), (quarter,)).astype(jnp.float32)
    scale = lax.dynamic_slice(w_out, (x * quarter,), (quarter,)).astype(jnp.float32)
    lists, w_a, w_b, tab = front(make_keys(indices, pool_len), w_first, tables)
    partial = lookup(lists.reshape(SRC, CAP), tab)
    return dense(partial, w_a, w_b, bias[None, :], scale[None, :]).reshape(128)


def solution(mesh):
    grid = Mesh(mesh.devices.reshape(2, 4, 4, 4), ALL)
    dev = ("x", "z", "y")
    placed = (
        P(ALL, None, None),
        P(),
        P(ALL, None),
        P(dev, "section"),
        P("section"),
        P("section"),
    )
    return jax.shard_map(body, mesh=grid, in_specs=placed, out_specs=P(dev), check_vma=False)
```

```python
import functools

import jax
import jax.numpy as jnp
from jax import lax
from jax.experimental import pallas as pl
from jax.experimental.pallas import tpu as pltpu
from jax.sharding import Mesh, PartitionSpec as P

TABLES = 32
SRC, BAGS, CAP = 128, 64, 512
TAIL = (16, 16, 16, 16, 32, 32)
G = 8
TB = 2048
NBUF = 4


def lookup_kernel(lists, tab, out, keys, rows_v, n_v, rows_s, n_s, buf, sem_n, sem_r, sem_f):
    y = lax.axis_index("y")
    lane = lax.broadcasted_iota(jnp.int32, (SRC, LANES), 1)
    blocks = [lists[:, b * LANES:(b + 1) * LANES] for b in range(BLKS)]
    first = sum(jnp.sum((v < (y << 21)).astype(jnp.int32), axis=1, keepdims=True) for v in blocks)
    blocks = rotate_left(blocks, lane, jnp.broadcast_to(first, (SRC, LANES)))
    n = jnp.zeros((SRC, 1), jnp.int32)
    for b in range(BLKS):
        mine = (blocks[b] >> 21) == y
        n += jnp.sum(mine.astype(jnp.int32), axis=1, keepdims=True)
        keys[:, b * LANES:(b + 1) * LANES] = jnp.where(mine, (blocks[b] >> 15) & 63, BAGS)
        rows_v[b] = jnp.where(mine, blocks[b] & 32767, 0)
    n_v[...] = jnp.broadcast_to(n, (SRC, LANES)).T[0:8]
    n_copy = pltpu.make_async_copy(n_v, n_s, sem_n)
    n_copy.start()

    def tile(r, grp, slot, sem):
        rows = pl.ds(pl.multiple_of(grp * G, G), G)
        return pltpu.make_async_copy(rows_v.at[r, rows, :], rows_s.at[slot, r], sem)

    for r in range(2):
        tile(r, 0, 0, sem_r.at[0, r]).start()
    buf[...] = jnp.zeros_like(buf)
    n_copy.wait()

    bag_row = lax.broadcasted_iota(jnp.int32, (BAGS, 256), 0)

    def part(grp, slot, g, lo):
        kk = keys[pl.ds(grp * G + g, 1), lo:lo + 256]
        oh = jnp.where(kk == bag_row, 1.0, 0.0).astype(jnp.bfloat16)
        return jnp.dot(oh, buf[slot, g, lo:lo + 256, :].astype(jnp.bfloat16), preferred_element_type=jnp.float32)

    def place(grp, g):
        return ((grp >> 1) & 1) * 64 + (grp & 1) * 8 + (grp >> 2) + (g % 4) * 16 + (g // 4) * 4

    def pool(grp, slot):
        for g in range(G):
            out[place(grp, g)] = part(grp, slot, g, 0).astype(jnp.bfloat16)

    def long_lists(grp, slot):
        most = n_s[0, grp * G]
        for g in range(1, G):
            most = jnp.maximum(most, n_s[0, grp * G + g])

        @pl.when(most > 256)
        def _():
            for r in (2, 3):
                copy = tile(r, grp, slot, sem_f)
                copy.start()
                copy.wait()

            for g in range(G):
                for r in (2, 3):
                    @pl.loop(0, 128)
                    def _(u):
                        buf[slot, g, pl.ds(r * 128 + u, 1), :] = tab[pl.ds(rows_s[slot, r, g, u], 1), :]
                total = part(grp, slot, g, 0) + part(grp, slot, g, 256)
                out[place(grp, g)] = total.astype(jnp.bfloat16)

    @pl.loop(0, SRC // G // 2)
    def _(h):
        for slot in range(2):
            grp = h * 2 + slot
            for r in range(2):
                tile(r, grp, slot, sem_r.at[slot, r]).wait()

            @pl.when(grp + 1 < SRC // G)
            def _():
                for r in range(2):
                    tile(r, grp + 1, 1 - slot, sem_r.at[1 - slot, r]).start()

            before = jnp.maximum(grp - 1, 0)
            for g in range(G):
                for u in range(128):
                    buf[slot, g, u:u + 1, :] = tab[pl.ds(rows_s[slot, 0, g, u], 1), :]
            pool(before, 1 - slot)
            for g in range(G):
                count = n_s[0, grp * G + g]
                at = 0
                for size in TAIL:
                    @pl.when(count > 128 + at)
                    def _(at=at, size=size):
                        for u in range(at, at + size):
                            buf[slot, g, 128 + u:129 + u, :] = tab[pl.ds(rows_s[slot, 1, g, u], 1), :]
                    at += size
            long_lists(before, 1 - slot)

    pool(SRC // G - 1, 1)
    long_lists(SRC // G - 1, 1)


def lookup(lists, tab):
    vmem = pl.BlockSpec(memory_space=pltpu.VMEM)
    return pl.pallas_call(
        lookup_kernel,
        out_shape=pltpu.VMEM((SRC, BAGS, 128), jnp.bfloat16),
        in_specs=[vmem, vmem],
        out_specs=vmem,
        scratch_shapes=[
            pltpu.VMEM((SRC, CAP), jnp.int32),
            pltpu.VMEM((4, SRC, 128), jnp.int32),
            pltpu.VMEM((8, 128), jnp.int32),
            pltpu.SMEM((2, 4, G, 128), jnp.int32),
            pltpu.SMEM((8, 128), jnp.int32),
            pltpu.VMEM((2, G, CAP, 128), jnp.float32),
            pltpu.SemaphoreType.DMA,
            pltpu.SemaphoreType.DMA((2, 2)),
            pltpu.SemaphoreType.DMA,
        ],
        compiler_params=pltpu.CompilerParams(vmem_limit_bytes=10 << 20),
        cost_estimate=pl.CostEstimate(flops=10**10, bytes_accessed=10**7, transcendentals=0),
    )(lists, tab)


LANES = 128
BLKS = CAP // LANES

def bitonic(xs, lane):
    pos = [lane + b * LANES for b in range(BLKS)]
    k = 2
    while k <= CAP:
        d = k // 2
        while d >= 1:
            if d >= LANES:
                step = d // LANES
                new = list(xs)
                for b in range(BLKS):
                    if b & step:
                        continue
                    lo, hi = jnp.minimum(xs[b], xs[b + step]), jnp.maximum(xs[b], xs[b + step])
                    up = ((b * LANES) & k) == 0
                    new[b], new[b + step] = (lo, hi) if up else (hi, lo)
                xs = new
            else:
                low = (lane & d) == 0
                new = []
                for b in range(BLKS):
                    x = xs[b]
                    other = jnp.where(low, pltpu.roll(x, LANES - d, 1), pltpu.roll(x, d, 1))
                    if k >= LANES:
                        up = ((b * LANES) & k) == 0
                        want_min = low if up else jnp.logical_not(low)
                    else:
                        want_min = ((pos[b] & k) == 0) == low
                    new.append(jnp.where(want_min, jnp.minimum(x, other), jnp.maximum(x, other)))
                xs = new
            d //= 2
        k *= 2
    return xs

def rotate_left(xs, lane, amount):
    s = 1
    while s < CAP:
        take = (amount & s) != 0
        if s >= LANES:
            step = s // LANES
            moved = [xs[(b + step) % BLKS] for b in range(BLKS)]
        else:
            rolled = [pltpu.roll(x, LANES - s, 1) for x in xs]
            moved = [jnp.where(lane < LANES - s, rolled[b], rolled[(b + 1) % BLKS]) for b in range(BLKS)]
        xs = [jnp.where(take, m, x) for m, x in zip(moved, xs)]
        s *= 2
    return xs

WZR, WZL, WYR, WYL, WFZR, WFZL, WFYR, WFYL = range(8)


def front_kernel(indices, pool_len, w, table, lists, w_a, w_b, tab, own, from_x, to_z, from_z, both, stage, xs, xr, ls, lr, gs, gr, sem_t):
    s = lax.axis_index("section")
    x = lax.axis_index("x")
    z = lax.axis_index("z")
    y = lax.axis_index("y")
    other = 1 - s
    nb = table.shape[0] // TB

    def fetch(i, slot):
        return pltpu.make_async_copy(table.at[pl.ds(i * TB, TB), :], stage.at[slot], sem_t.at[slot])

    for i in range(NBUF):
        fetch(i, i).start()

    def widen(h):
        @pl.loop(h * (nb // NBUF) // 4, (h + 1) * (nb // NBUF) // 4)
        def _(k):
            for slot in range(NBUF):
                i = k * NBUF + slot
                fetch(i, slot).wait()
                tab[pl.ds(pl.multiple_of(i * TB, TB), TB), :] = stage[slot].astype(jnp.float32)

                @pl.when(i + NBUF < nb)
                def _():
                    fetch(i + NBUF, slot).start()

    barrier = pltpu.get_barrier_semaphore()
    peers = [{"section": other}]
    for axis, at in (("x", x), ("z", z), ("y", y)):
        peers += [{axis: lax.rem(at + d, 4)} for d in (1, 2, 3)]
    for peer in peers:
        pl.semaphore_signal(barrier, inc=1, device_id=peer, device_id_type=MESH)

    lane = lax.broadcasted_iota(jnp.int32, (TABLES, LANES), 1)
    row = lax.broadcasted_iota(jnp.int32, (TABLES, TABLES), 0)
    column = lax.broadcasted_iota(jnp.int32, (TABLES, TABLES), 1)
    used = jnp.sum(jnp.where(row == column, jnp.broadcast_to(pool_len[...], (TABLES, TABLES)), 0), axis=1, keepdims=True)
    blocks = []
    for b in range(BLKS):
        idx = jnp.concatenate([indices[:, 2 * b, :], indices[:, 2 * b + 1, :]], axis=1)
        slot = 2 * b + (lane >> 6)
        key = ((idx >> 15) << 21) | ((lane & 63) << 15) | (idx & 32767)
        blocks.append(jnp.where(slot < used, key, 4 << 21))
    blocks = bitonic(blocks, lane)
    for b in range(BLKS):
        for xi in range(4):
            for si in range(2):
                t = si * 16 + xi * 4
                own[xi, si * 4:si * 4 + 4, b * LANES:(b + 1) * LANES] = blocks[b][t:t + 4]
    pl.semaphore_wait(barrier, len(peers))

    def list_copy(k, src, dst, peer):
        return pltpu.make_async_remote_copy(
            src_ref=src, dst_ref=dst, send_sem=ls.at[k], recv_sem=lr.at[k], device_id=peer, device_id_type=MESH,
        )

    sent = []
    along_x = []
    for i in range(3):
        to = lax.rem(x + i + 1, 4)
        along_x.append(list_copy(i, own.at[to], from_x.at[x], {"x": to}))
    for copy in along_x:
        copy.start()

    x_copies = []
    for i in range(3):
        to = lax.rem(x + i + 1, 4)
        for half, full, mine in ((0, w_a, z), (1, w_b, y)):
            cols = pl.ds(pl.multiple_of(to * 512 + half * 256, 256), 256)
            copy = pltpu.make_async_remote_copy(
                src_ref=w.at[:, cols], dst_ref=full.at[mine, x], send_sem=xs.at[i, half], recv_sem=xr.at[i, half],
                device_id={"x": to}, device_id_type=MESH,
            )
            copy.start()
            x_copies.append(copy)
    for half, full, mine in ((0, w_a, z), (1, w_b, y)):
        cols = pl.ds(pl.multiple_of(x * 512 + half * 256, 256), 256)
        full[mine, x] = w[:, cols]
    from_x[x] = own[x]
    widen(0)

    def ring(kind, ref, axis, to):
        return pltpu.make_async_remote_copy(
            src_ref=ref, dst_ref=ref, send_sem=gs.at[kind], recv_sem=gr.at[kind], device_id={axis: to}, device_id_type=MESH,
        )

    z_right, z_left = lax.rem(z + 1, 4), lax.rem(z + 3, 4)
    y_right, y_left = lax.rem(y + 1, 4), lax.rem(y + 3, 4)
    low, high = pl.ds(0, 2), pl.ds(2, 2)
    near = [
        ring(WZR, w_a.at[z], "z", z_right), ring(WZL, w_a.at[z], "z", z_left),
        ring(WYR, w_b.at[y], "y", y_right), ring(WYL, w_b.at[y], "y", y_left),
    ]
    far = [
        ring(WFZR, w_a.at[z_left, low], "z", z_right), ring(WFZL, w_a.at[z_right, high], "z", z_left),
        ring(WFYR, w_b.at[y_left, low], "y", y_right), ring(WFYL, w_b.at[y_right, high], "y", y_left),
    ]
    for copy in along_x:
        copy.wait_recv()
    for xi in range(4):
        for si in range(2):
            for zi in range(4):
                to_z[zi, si * 4 + xi:si * 4 + xi + 1, :] = from_x[xi, si * 4 + zi:si * 4 + zi + 1, :]
    along_z = []
    for i in range(3):
        to = lax.rem(z + i + 1, 4)
        along_z.append(list_copy(3 + i, to_z.at[to], from_z.at[z], {"z": to}))
    for copy in along_z:
        copy.start()
    from_z[z] = to_z[z]
    for copy in x_copies:
        copy.wait_recv()
    for copy in near:
        copy.start()
    widen(1)

    for copy in along_z:
        copy.wait_recv()
    for zi in range(4):
        for si in range(2):
            both[si, zi * 4:zi * 4 + 4, :] = from_z[zi, si * 4:si * 4 + 4, :]
    across = list_copy(6, both.at[other], lists.at[y, s], {"section": other})
    across.start()
    along_y = []
    for i in range(3):
        along_y.append(list_copy(7 + i, both.at[s], lists.at[y, s], {"y": lax.rem(y + i + 1, 4)}))
    for copy in along_y:
        copy.start()
    lists[y, s] = both[s]
    across.wait_recv()
    for i in range(3):
        copy = list_copy(10 + i, lists.at[y, other], lists.at[y, other], {"y": lax.rem(y + i + 1, 4)})
        copy.start()
        along_y.append(copy)

    widen(2)
    for copy, onward in zip(near, far):
        copy.wait_recv()
        onward.start()
    widen(3)
    for copy in along_y + far:
        copy.wait_recv()
    for copy in along_x + along_z + [across] + along_y + x_copies + near + far:
        copy.wait_send()


def front(indices, pool_len, w, table):
    vmem = pl.BlockSpec(memory_space=pltpu.VMEM)
    piece = pltpu.VMEM((4, 4, 64, 256), jnp.bfloat16)
    rows = pltpu.VMEM((4, 8, CAP), jnp.int32)
    dma = pltpu.SemaphoreType.DMA
    return pl.pallas_call(
        front_kernel,
        out_shape=(
            pltpu.VMEM((4, 2, 16, CAP), jnp.int32), piece, piece, pltpu.VMEM(table.shape, jnp.float32),
        ),
        in_specs=[vmem, vmem, vmem, pl.BlockSpec(memory_space=pl.ANY)],
        out_specs=(vmem,) * 4,
        scratch_shapes=[
            rows, rows, rows, rows,
            pltpu.VMEM((2, 16, CAP), jnp.int32),
            pltpu.VMEM((NBUF, TB, 128), jnp.bfloat16),
            dma((3, 2)), dma((3, 2)), dma((13,)), dma((13,)), dma((8,)), dma((8,)), dma((NBUF,)),
        ],
        compiler_params=pltpu.CompilerParams(collective_id=0, has_side_effects=True, vmem_limit_bytes=44 << 20),
        cost_estimate=pl.CostEstimate(flops=10**10, bytes_accessed=10**7, transcendentals=0),
    )(jnp.transpose(indices, (1, 2, 0)), pool_len[None, :], w, table)


MESH = pl.DeviceIdType.MESH
C = 4
(FAR_A, FAR_B, SUM_A, SUM_B, NEAR_A, NEAR_B, Z1, Z2, Z3, XR, XL, FWD_A, FWD_B, OWN_S, LEFT_S, RIGHT_S, FAR_SA, FAR_SB) = range(18)
KINDS = 18


def dense_kernel(part, w_a, w_b, a_left, b_left, bias, scale, out, mid_a, mid_b, from_l, from_r, pooled, feats, acc, plog, lrecv, full_a, full_b, ssem, rsem, lsend, lrec, wsend, wrecv):
    s = lax.axis_index("section")
    x = lax.axis_index("x")
    z = lax.axis_index("z")
    y = lax.axis_index("y")
    right_y, left_y, far_y = lax.rem(y + 1, 4), lax.rem(y + 3, 4), lax.rem(y + 2, 4)
    right_x, left_x, far_x = lax.rem(x + 1, 4), lax.rem(x + 3, 4), lax.rem(x + 2, 4)
    other = 1 - s

    barrier = pltpu.get_barrier_semaphore()
    peers = [{"y": right_y}, {"y": left_y}]
    peers += [{"z": lax.rem(z + d, 4)} for d in (1, 2, 3)]
    peers += [{"x": lax.rem(x + d, 4)} for d in (1, 2, 3)]
    peers += [{"section": other}]
    peers += [{"section": other, "x": lax.rem(x + d, 4)} for d in (1, 2, 3)]
    for peer in peers:
        pl.semaphore_signal(barrier, inc=1, device_id=peer, device_id_type=MESH)
    pl.semaphore_wait(barrier, len(peers))

    def remote(src, dst, kind, c, peer):
        return pltpu.make_async_remote_copy(
            src_ref=src, dst_ref=dst, send_sem=ssem.at[kind, c], recv_sem=rsem.at[kind, c],
            device_id=peer, device_id_type=MESH,
        )

    A, B = pl.ds(0, 2), pl.ds(2, 2)
    copies = []
    for c in range(C):
        one = {
            FAR_A: remote(part.at[c, A, far_y], mid_a.at[c], FAR_A, c, {"y": right_y}),
            FAR_B: remote(part.at[c, B, far_y], mid_b.at[c], FAR_B, c, {"y": left_y}),
            SUM_A: remote(mid_a.at[c], from_l.at[c, A], SUM_A, c, {"y": right_y}),
            SUM_B: remote(mid_b.at[c], from_r.at[c, B], SUM_B, c, {"y": left_y}),
            NEAR_B: remote(part.at[c, B, right_y], from_l.at[c, B], NEAR_B, c, {"y": right_y}),
            NEAR_A: remote(part.at[c, A, left_y], from_r.at[c, A], NEAR_A, c, {"y": left_y}),
            XR: remote(feats.at[s, x, c], feats.at[s, x, c], XR, c, {"x": right_x}),
            XL: remote(feats.at[s, x, c], feats.at[s, x, c], XL, c, {"x": left_x}),
            FWD_A: remote(feats.at[s, left_x, c, A], feats.at[s, left_x, c, A], FWD_A, c, {"x": right_x}),
            FWD_B: remote(feats.at[s, right_x, c, B], feats.at[s, right_x, c, B], FWD_B, c, {"x": left_x}),
            OWN_S: remote(feats.at[s, x, c], feats.at[s, x, c], OWN_S, c, {"section": other}),
            LEFT_S: remote(feats.at[s, left_x, c], feats.at[s, left_x, c], LEFT_S, c, {"section": other}),
            RIGHT_S: remote(feats.at[s, right_x, c], feats.at[s, right_x, c], RIGHT_S, c, {"section": other}),
            FAR_SA: remote(feats.at[s, far_x, c, A], feats.at[s, far_x, c, A], FAR_SA, c, {"section": other}),
            FAR_SB: remote(feats.at[s, far_x, c, B], feats.at[s, far_x, c, B], FAR_SB, c, {"section": other}),
        }
        for i, kind in enumerate((Z1, Z2, Z3)):
            to = lax.rem(z + i + 1, 4)
            one[kind] = remote(pooled.at[c, to], feats.at[s, x, c, z], kind, c, {"z": to})
        copies.append(one)

    def start(c, *kinds):
        for kind in kinds:
            copies[c][kind].start()

    def arrive(c, *kinds):
        for kind in kinds:
            copies[c][kind].wait_recv()

    right_z, left_z = lax.rem(z + 1, 4), lax.rem(z + 3, 4)

    def w_copies(k, src, full, row, axis, to):
        return [
            pltpu.make_async_remote_copy(
                src_ref=src.at[i], dst_ref=full.at[row, i], send_sem=wsend.at[k, i], recv_sem=wrecv.at[k, i],
                device_id={axis: to}, device_id_type=MESH,
            )
            for i in range(4)
        ]

    w_y = [w_copies(0, w_a, full_a, y, "y", left_y), w_copies(1, a_left, full_a, left_y, "y", right_y)]
    w_z = [w_copies(2, w_b, full_b, z, "z", left_z), w_copies(3, b_left, full_b, left_z, "z", right_z)]

    def w_start(both, *pieces):
        for i in pieces:
            both[0][i].start()
            both[1][i].start()

    def stage_far(c):
        start(c, FAR_A, FAR_B)

    def stage_sum(c):
        arrive(c, FAR_A)
        mid_a[c] = (mid_a[c].astype(jnp.float32) + part[c, 0:2, right_y].astype(jnp.float32)).astype(jnp.bfloat16)
        start(c, SUM_A)
        arrive(c, FAR_B)
        mid_b[c] = (mid_b[c].astype(jnp.float32) + part[c, 2:4, left_y].astype(jnp.float32)).astype(jnp.bfloat16)
        start(c, SUM_B)
        start(c, NEAR_B, NEAR_A)
        if c + 2 < C:
            stage_far(c + 2)

    def stage_pool(c):
        arrive(c, SUM_A, NEAR_B, SUM_B, NEAR_A)
        total = part[c, :, y].astype(jnp.float32) + from_l[c].astype(jnp.float32) + from_r[c].astype(jnp.float32)
        pooled[c] = total.astype(jnp.bfloat16)
        start(c, Z1, Z3, Z2)
        feats[s, x, c, z] = pooled[c, z]

    def stage_x(c):
        arrive(c, Z1, Z3, Z2)
        start(c, XR, XL, OWN_S)

    def stage_fwd(c):
        arrive(c, XR)
        start(c, FWD_A, LEFT_S)
        arrive(c, XL)
        start(c, FWD_B, RIGHT_S)

    def stage_far_s(c):
        arrive(c, FWD_A)
        start(c, FAR_SA)
        arrive(c, FWD_B)
        start(c, FAR_SB)

    columns = pl.ds(pl.multiple_of(x * 512, 512), 512)
    bias_row = bias[:, columns].astype(jnp.float32)
    scale_row = scale[:, columns].astype(jnp.float32)

    def dense_rows(first, last):
        rows = (last - first) * 128
        for c in range(first, last):
            arrive(c, OWN_S, LEFT_S, RIGHT_S, FAR_SA, FAR_SB)
        acc[0:rows] = jnp.zeros((rows, 512), jnp.float32)

        @pl.loop(0, 8)
        def _(i):
            si, xi = i // 4, lax.rem(i, 4)
            zi, wx = 2 * lax.rem(i, 2), i // 2
            lhs = jnp.concatenate(
                [jnp.concatenate([feats[si, xi, c, j] for j in range(4)], axis=1) for c in range(first, last)], axis=0
            )
            rhs_a = jnp.concatenate([full_a[yy, zi + zz, wx] for zz in range(2) for yy in range(4)], axis=0)
            acc[0:rows, 0:256] += jnp.dot(lhs, rhs_a, preferred_element_type=jnp.float32)
            rhs_b = jnp.concatenate([full_b[zi + zz, yy, wx] for zz in range(2) for yy in range(4)], axis=0)
            acc[0:rows, 256:512] += jnp.dot(lhs, rhs_b, preferred_element_type=jnp.float32)

        for k in range(rows // 128):
            h = jnp.maximum(acc[k * 128:(k + 1) * 128] + bias_row, 0.0) * scale_row
            h = h[:, 0:128] + h[:, 128:256] + h[:, 256:384] + h[:, 384:512]
            plog[first + k] = jnp.sum(h.T, axis=0, keepdims=True)

    stage_far(0)
    stage_far(1)
    w_start(w_z, 0, 1)
    full_a[y] = w_a[...]
    full_a[left_y] = a_left[...]
    full_b[z] = w_b[...]
    full_b[left_z] = b_left[...]
    stages = (stage_sum, stage_pool, stage_x, stage_fwd, stage_far_s)
    for step in range(C + len(stages) - 1):
        if step == C + 3:
            for copy in sum(w_y + w_z, []):
                copy.wait_recv()
            dense_rows(0, 3)
        for i, stage in enumerate(stages):
            if 0 <= step - i < C:
                stage(step - i)
        if step == 1:
            w_start(w_z, 2)
        elif step == 2:
            w_start(w_z, 3)
        elif step == 3:
            w_start(w_y, 0, 1, 2, 3)
    dense_rows(3, 4)

    sent = []
    for ds in range(2):
        for dx in range(4):
            if ds == 0 and dx == 0:
                continue
            to_s = s if ds == 0 else other
            to_x = lax.rem(x + dx, 4)
            k = ds * 4 + dx
            copy = pltpu.make_async_remote_copy(
                src_ref=plog.at[to_x], dst_ref=lrecv.at[s * 4 + x], send_sem=lsend.at[k], recv_sem=lrec.at[k],
                device_id={"section": to_s, "x": to_x}, device_id_type=MESH,
            )
            copy.start()
            sent.append(copy)
    lrecv[s * 4 + x] = plog[x]
    for copy in sent:
        copy.wait_recv()
    total = lrecv[0]
    for i in range(1, 8):
        total = total + lrecv[i]
    out[...] = total
    for copy in sent + sum(w_y + w_z, []):
        copy.wait_send()
    for c in range(C):
        for kind in range(KINDS):
            copies[c][kind].wait_send()


def dense(partial, weights, bias, scale):
    bf = jnp.bfloat16
    vmem = pl.BlockSpec(memory_space=pltpu.VMEM)
    return pl.pallas_call(
        dense_kernel,
        out_shape=jax.ShapeDtypeStruct((1, 128), jnp.float32),
        in_specs=[vmem] * 7,
        out_specs=vmem,
        scratch_shapes=[
            pltpu.VMEM((C, 2, 128, 128), bf),
            pltpu.VMEM((C, 2, 128, 128), bf),
            pltpu.VMEM((C, 4, 128, 128), bf),
            pltpu.VMEM((C, 4, 128, 128), bf),
            pltpu.VMEM((C, 4, 128, 128), bf),
            pltpu.VMEM((2, 4, C, 4, 128, 128), bf),
            pltpu.VMEM((384, 512), jnp.float32),
            pltpu.VMEM((C, 1, 128), jnp.float32),
            pltpu.VMEM((8, 1, 128), jnp.float32),
            pltpu.VMEM((4, 4, 4, 64, 256), bf),
            pltpu.VMEM((4, 4, 4, 64, 256), bf),
            pltpu.SemaphoreType.DMA((KINDS, C)),
            pltpu.SemaphoreType.DMA((KINDS, C)),
            pltpu.SemaphoreType.DMA((8,)),
            pltpu.SemaphoreType.DMA((8,)),
            pltpu.SemaphoreType.DMA((4, 4)),
            pltpu.SemaphoreType.DMA((4, 4)),
        ],
        compiler_params=pltpu.CompilerParams(collective_id=1, has_side_effects=True, vmem_limit_bytes=20 << 20),
        cost_estimate=pl.CostEstimate(flops=3 * 10**10, bytes_accessed=10**7, transcendentals=0),
    )(partial.reshape(4, 4, 4, 128, 128), *weights, bias, scale)


ALL = ("section", "x", "z", "y")


def body(indices, pool_len, tables, w_first, b_first, w_out):
    lists, w_a, w_b, tab = front(indices, pool_len, w_first, tables)
    up = [(i, (i + 1) % 4) for i in range(4)]
    weights = [w_a, w_b, lax.ppermute(w_a, "y", up), lax.ppermute(w_b, "z", up)]
    partial = lookup(lists.reshape(SRC, CAP), tab)
    return dense(partial, weights, b_first[None, :], w_out[None, :]).reshape(128)


def solution(mesh):
    grid = Mesh(mesh.devices.reshape(2, 4, 4, 4), ALL)
    dev = ("x", "z", "y")
    placed = (
        P(ALL, None, None),
        P(),
        P(ALL, None),
        P(dev, "section"),
        P("section"),
        P("section"),
    )
    return jax.shard_map(body, mesh=grid, in_specs=placed, out_specs=P(dev), check_vma=False)
```

```python
import functools

import jax
import jax.numpy as jnp
from jax import lax
from jax.experimental import pallas as pl
from jax.experimental.pallas import tpu as pltpu
from jax.sharding import Mesh, PartitionSpec as P

TABLES = 32
SRC, BAGS, CAP = 128, 64, 512
TAIL = (16, 16, 16, 16, 32, 32)
G = 8
TB = 2048
NBUF = 4


def lookup_kernel(lists, tab, out, keys, rows_v, n_v, rows_s, n_s, buf, sem_n, sem_r, sem_f):
    y = lax.axis_index("y")
    lane = lax.broadcasted_iota(jnp.int32, (SRC, LANES), 1)
    blocks = [lists[:, b * LANES:(b + 1) * LANES] for b in range(BLKS)]
    first = sum(jnp.sum((v < (y << 21)).astype(jnp.int32), axis=1, keepdims=True) for v in blocks)
    blocks = rotate_left(blocks, lane, jnp.broadcast_to(first, (SRC, LANES)))
    n = jnp.zeros((SRC, 1), jnp.int32)
    for b in range(BLKS):
        mine = (blocks[b] >> 21) == y
        n += jnp.sum(mine.astype(jnp.int32), axis=1, keepdims=True)
        keys[:, b * LANES:(b + 1) * LANES] = jnp.where(mine, (blocks[b] >> 15) & 63, BAGS)
        rows_v[b] = jnp.where(mine, blocks[b] & 32767, 0)
    n_v[...] = jnp.broadcast_to(n, (SRC, LANES)).T[0:8]
    n_copy = pltpu.make_async_copy(n_v, n_s, sem_n)
    n_copy.start()

    def tile(r, grp, slot, sem):
        rows = pl.ds(pl.multiple_of(grp * G, G), G)
        return pltpu.make_async_copy(rows_v.at[r, rows, :], rows_s.at[slot, r], sem)

    for r in range(2):
        tile(r, 0, 0, sem_r.at[0, r]).start()
    buf[...] = jnp.zeros_like(buf)
    n_copy.wait()

    bag_row = lax.broadcasted_iota(jnp.int32, (BAGS, 256), 0)

    def part(grp, slot, g, lo):
        kk = keys[pl.ds(grp * G + g, 1), lo:lo + 256]
        oh = jnp.where(kk == bag_row, 1.0, 0.0).astype(jnp.bfloat16)
        return jnp.dot(oh, buf[slot, g, lo:lo + 256, :].astype(jnp.bfloat16), preferred_element_type=jnp.float32)

    def place(grp, g):
        return ((grp >> 1) & 1) * 64 + (grp & 1) * 8 + (grp >> 2) + (g % 4) * 16 + (g // 4) * 4

    def pool(grp, slot):
        for g in range(G):
            out[place(grp, g)] = part(grp, slot, g, 0).astype(jnp.bfloat16)

    def long_lists(grp, slot):
        most = n_s[0, grp * G]
        for g in range(1, G):
            most = jnp.maximum(most, n_s[0, grp * G + g])

        @pl.when(most > 256)
        def _():
            for r in (2, 3):
                copy = tile(r, grp, slot, sem_f)
                copy.start()
                copy.wait()

            for g in range(G):
                for r in (2, 3):
                    @pl.loop(0, 128)
                    def _(u):
                        buf[slot, g, pl.ds(r * 128 + u, 1), :] = tab[pl.ds(rows_s[slot, r, g, u], 1), :]
                total = part(grp, slot, g, 0) + part(grp, slot, g, 256)
                out[place(grp, g)] = total.astype(jnp.bfloat16)

    def tail(count, slot, g, at, sizes):
        @pl.when(count > at)
        def _():
            for u in range(at, at + sizes[0]):
                buf[slot, g, u:u + 1, :] = tab[pl.ds(rows_s[slot, 1, g, u - 128], 1), :]
            if len(sizes) > 1:
                tail(count, slot, g, at + sizes[0], sizes[1:])

    @pl.loop(0, SRC // G // 2)
    def _(h):
        for slot in range(2):
            grp = h * 2 + slot
            for r in range(2):
                tile(r, grp, slot, sem_r.at[slot, r]).wait()

            @pl.when(grp + 1 < SRC // G)
            def _():
                for r in range(2):
                    tile(r, grp + 1, 1 - slot, sem_r.at[1 - slot, r]).start()

            before = jnp.maximum(grp - 1, 0)
            for g in range(G):
                for u in range(128):
                    buf[slot, g, u:u + 1, :] = tab[pl.ds(rows_s[slot, 0, g, u], 1), :]
            pool(before, 1 - slot)
            for g in range(G):
                tail(n_s[0, grp * G + g], slot, g, 128, TAIL)
            long_lists(before, 1 - slot)

    pool(SRC // G - 1, 1)
    long_lists(SRC // G - 1, 1)


def lookup(lists, tab):
    vmem = pl.BlockSpec(memory_space=pltpu.VMEM)
    return pl.pallas_call(
        lookup_kernel,
        out_shape=pltpu.VMEM((SRC, BAGS, 128), jnp.bfloat16),
        in_specs=[vmem, vmem],
        out_specs=vmem,
        scratch_shapes=[
            pltpu.VMEM((SRC, CAP), jnp.int32),
            pltpu.VMEM((4, SRC, 128), jnp.int32),
            pltpu.VMEM((8, 128), jnp.int32),
            pltpu.SMEM((2, 4, G, 128), jnp.int32),
            pltpu.SMEM((8, 128), jnp.int32),
            pltpu.VMEM((2, G, CAP, 128), jnp.float32),
            pltpu.SemaphoreType.DMA,
            pltpu.SemaphoreType.DMA((2, 2)),
            pltpu.SemaphoreType.DMA,
        ],
        compiler_params=pltpu.CompilerParams(vmem_limit_bytes=10 << 20),
        cost_estimate=pl.CostEstimate(flops=10**10, bytes_accessed=10**7, transcendentals=0),
    )(lists, tab)


LANES = 128
BLKS = CAP // LANES

def bitonic(xs, lane):
    pos = [lane + b * LANES for b in range(BLKS)]
    k = 2
    while k <= CAP:
        d = k // 2
        while d >= 1:
            if d >= LANES:
                step = d // LANES
                new = list(xs)
                for b in range(BLKS):
                    if b & step:
                        continue
                    lo, hi = jnp.minimum(xs[b], xs[b + step]), jnp.maximum(xs[b], xs[b + step])
                    up = ((b * LANES) & k) == 0
                    new[b], new[b + step] = (lo, hi) if up else (hi, lo)
                xs = new
            else:
                low = (lane & d) == 0
                new = []
                for b in range(BLKS):
                    x = xs[b]
                    other = jnp.where(low, pltpu.roll(x, LANES - d, 1), pltpu.roll(x, d, 1))
                    if k >= LANES:
                        up = ((b * LANES) & k) == 0
                        want_min = low if up else jnp.logical_not(low)
                    else:
                        want_min = ((pos[b] & k) == 0) == low
                    new.append(jnp.where(want_min, jnp.minimum(x, other), jnp.maximum(x, other)))
                xs = new
            d //= 2
        k *= 2
    return xs

def rotate_left(xs, lane, amount):
    s = 1
    while s < CAP:
        take = (amount & s) != 0
        if s >= LANES:
            step = s // LANES
            moved = [xs[(b + step) % BLKS] for b in range(BLKS)]
        else:
            rolled = [pltpu.roll(x, LANES - s, 1) for x in xs]
            moved = [jnp.where(lane < LANES - s, rolled[b], rolled[(b + 1) % BLKS]) for b in range(BLKS)]
        xs = [jnp.where(take, m, x) for m, x in zip(moved, xs)]
        s *= 2
    return xs

WZR, WZL, WYR, WYL, WFZR, WFZL, WFYR, WFYL = range(8)


def front_kernel(indices, pool_len, w, table, lists, w_a, w_b, tab, own, from_x, to_z, from_z, both, stage, xs, xr, ls, lr, gs, gr, sem_t):
    s = lax.axis_index("section")
    x = lax.axis_index("x")
    z = lax.axis_index("z")
    y = lax.axis_index("y")
    other = 1 - s
    nb = table.shape[0] // TB

    def fetch(i, slot):
        return pltpu.make_async_copy(table.at[pl.ds(i * TB, TB), :], stage.at[slot], sem_t.at[slot])

    for i in range(NBUF):
        fetch(i, i).start()

    def widen(h):
        @pl.loop(h * (nb // NBUF) // 4, (h + 1) * (nb // NBUF) // 4)
        def _(k):
            for slot in range(NBUF):
                i = k * NBUF + slot
                fetch(i, slot).wait()
                tab[pl.ds(pl.multiple_of(i * TB, TB), TB), :] = stage[slot].astype(jnp.float32)

                @pl.when(i + NBUF < nb)
                def _():
                    fetch(i + NBUF, slot).start()

    barrier = pltpu.get_barrier_semaphore()
    peers = [{"section": other}]
    for axis, at in (("x", x), ("z", z), ("y", y)):
        peers += [{axis: lax.rem(at + d, 4)} for d in (1, 2, 3)]
    for peer in peers:
        pl.semaphore_signal(barrier, inc=1, device_id=peer, device_id_type=MESH)

    lane = lax.broadcasted_iota(jnp.int32, (TABLES, LANES), 1)
    row = lax.broadcasted_iota(jnp.int32, (TABLES, TABLES), 0)
    column = lax.broadcasted_iota(jnp.int32, (TABLES, TABLES), 1)
    used = jnp.sum(jnp.where(row == column, jnp.broadcast_to(pool_len[...], (TABLES, TABLES)), 0), axis=1, keepdims=True)
    blocks = []
    for b in range(BLKS):
        idx = jnp.concatenate([indices[:, 2 * b, :], indices[:, 2 * b + 1, :]], axis=1)
        slot = 2 * b + (lane >> 6)
        key = ((idx >> 15) << 21) | ((lane & 63) << 15) | (idx & 32767)
        blocks.append(jnp.where(slot < used, key, 4 << 21))
    blocks = bitonic(blocks, lane)
    for b in range(BLKS):
        for xi in range(4):
            for si in range(2):
                t = si * 16 + xi * 4
                own[xi, si * 4:si * 4 + 4, b * LANES:(b + 1) * LANES] = blocks[b][t:t + 4]
    pl.semaphore_wait(barrier, len(peers))

    def list_copy(k, src, dst, peer):
        return pltpu.make_async_remote_copy(
            src_ref=src, dst_ref=dst, send_sem=ls.at[k], recv_sem=lr.at[k], device_id=peer, device_id_type=MESH,
        )

    sent = []
    along_x = []
    for i in range(3):
        to = lax.rem(x + i + 1, 4)
        along_x.append(list_copy(i, own.at[to], from_x.at[x], {"x": to}))
    for copy in along_x:
        copy.start()

    x_copies = []
    for i in range(3):
        to = lax.rem(x + i + 1, 4)
        for half, full, mine in ((0, w_a, z), (1, w_b, y)):
            cols = pl.ds(pl.multiple_of(to * 512 + half * 256, 256), 256)
            copy = pltpu.make_async_remote_copy(
                src_ref=w.at[:, cols], dst_ref=full.at[mine, x], send_sem=xs.at[i, half], recv_sem=xr.at[i, half],
                device_id={"x": to}, device_id_type=MESH,
            )
            copy.start()
            x_copies.append(copy)
    for half, full, mine in ((0, w_a, z), (1, w_b, y)):
        cols = pl.ds(pl.multiple_of(x * 512 + half * 256, 256), 256)
        full[mine, x] = w[:, cols]
    from_x[x] = own[x]
    widen(0)

    def ring(kind, ref, axis, to):
        return pltpu.make_async_remote_copy(
            src_ref=ref, dst_ref=ref, send_sem=gs.at[kind], recv_sem=gr.at[kind], device_id={axis: to}, device_id_type=MESH,
        )

    z_right, z_left = lax.rem(z + 1, 4), lax.rem(z + 3, 4)
    y_right, y_left = lax.rem(y + 1, 4), lax.rem(y + 3, 4)
    low, high = pl.ds(0, 2), pl.ds(2, 2)
    near = [
        ring(WZR, w_a.at[z], "z", z_right), ring(WZL, w_a.at[z], "z", z_left),
        ring(WYR, w_b.at[y], "y", y_right), ring(WYL, w_b.at[y], "y", y_left),
    ]
    far = [
        ring(WFZR, w_a.at[z_left, low], "z", z_right), ring(WFZL, w_a.at[z_right, high], "z", z_left),
        ring(WFYR, w_b.at[y_left, low], "y", y_right), ring(WFYL, w_b.at[y_right, high], "y", y_left),
    ]
    for copy in along_x:
        copy.wait_recv()
    for xi in range(4):
        for si in range(2):
            for zi in range(4):
                to_z[zi, si * 4 + xi:si * 4 + xi + 1, :] = from_x[xi, si * 4 + zi:si * 4 + zi + 1, :]
    along_z = []
    for i in range(3):
        to = lax.rem(z + i + 1, 4)
        along_z.append(list_copy(3 + i, to_z.at[to], from_z.at[z], {"z": to}))
    for copy in along_z:
        copy.start()
    from_z[z] = to_z[z]
    for copy in x_copies:
        copy.wait_recv()
    for copy in near:
        copy.start()
    widen(1)

    for copy in along_z:
        copy.wait_recv()
    for zi in range(4):
        for si in range(2):
            both[si, zi * 4:zi * 4 + 4, :] = from_z[zi, si * 4:si * 4 + 4, :]
    across = list_copy(6, both.at[other], lists.at[y, s], {"section": other})
    across.start()
    along_y = []
    for i in range(3):
        along_y.append(list_copy(7 + i, both.at[s], lists.at[y, s], {"y": lax.rem(y + i + 1, 4)}))
    for copy in along_y:
        copy.start()
    lists[y, s] = both[s]
    across.wait_recv()
    for i in range(3):
        copy = list_copy(10 + i, lists.at[y, other], lists.at[y, other], {"y": lax.rem(y + i + 1, 4)})
        copy.start()
        along_y.append(copy)

    widen(2)
    for copy, onward in zip(near, far):
        copy.wait_recv()
        onward.start()
    widen(3)
    for copy in along_y + far:
        copy.wait_recv()
    for copy in along_x + along_z + [across] + along_y + x_copies + near + far:
        copy.wait_send()


def front(indices, pool_len, w, table):
    vmem = pl.BlockSpec(memory_space=pltpu.VMEM)
    piece = pltpu.VMEM((4, 4, 64, 256), jnp.bfloat16)
    rows = pltpu.VMEM((4, 8, CAP), jnp.int32)
    dma = pltpu.SemaphoreType.DMA
    return pl.pallas_call(
        front_kernel,
        out_shape=(
            pltpu.VMEM((4, 2, 16, CAP), jnp.int32), piece, piece, pltpu.VMEM(table.shape, jnp.float32),
        ),
        in_specs=[vmem, vmem, vmem, pl.BlockSpec(memory_space=pl.ANY)],
        out_specs=(vmem,) * 4,
        scratch_shapes=[
            rows, rows, rows, rows,
            pltpu.VMEM((2, 16, CAP), jnp.int32),
            pltpu.VMEM((NBUF, TB, 128), jnp.bfloat16),
            dma((3, 2)), dma((3, 2)), dma((13,)), dma((13,)), dma((8,)), dma((8,)), dma((NBUF,)),
        ],
        compiler_params=pltpu.CompilerParams(collective_id=0, has_side_effects=True, vmem_limit_bytes=44 << 20),
        cost_estimate=pl.CostEstimate(flops=10**10, bytes_accessed=10**7, transcendentals=0),
    )(jnp.transpose(indices, (1, 2, 0)), pool_len[None, :], w, table)


MESH = pl.DeviceIdType.MESH
C = 4
(FAR_A, FAR_B, SUM_A, SUM_B, NEAR_A, NEAR_B, Z1, Z2, Z3, XR, XL, FWD_A, FWD_B, OWN_S, LEFT_S, RIGHT_S, FAR_SA, FAR_SB) = range(18)
KINDS = 18


def dense_kernel(part, w_a, w_b, a_left, b_left, bias, scale, out, mid_a, mid_b, from_l, from_r, pooled, feats, acc, plog, lrecv, full_a, full_b, ssem, rsem, lsend, lrec, wsend, wrecv):
    s = lax.axis_index("section")
    x = lax.axis_index("x")
    z = lax.axis_index("z")
    y = lax.axis_index("y")
    right_y, left_y, far_y = lax.rem(y + 1, 4), lax.rem(y + 3, 4), lax.rem(y + 2, 4)
    right_x, left_x, far_x = lax.rem(x + 1, 4), lax.rem(x + 3, 4), lax.rem(x + 2, 4)
    other = 1 - s

    barrier = pltpu.get_barrier_semaphore()
    peers = [{"y": right_y}, {"y": left_y}]
    peers += [{"z": lax.rem(z + d, 4)} for d in (1, 2, 3)]
    peers += [{"x": lax.rem(x + d, 4)} for d in (1, 2, 3)]
    peers += [{"section": other}]
    peers += [{"section": other, "x": lax.rem(x + d, 4)} for d in (1, 2, 3)]
    for peer in peers:
        pl.semaphore_signal(barrier, inc=1, device_id=peer, device_id_type=MESH)
    pl.semaphore_wait(barrier, len(peers))

    def remote(src, dst, kind, c, peer):
        return pltpu.make_async_remote_copy(
            src_ref=src, dst_ref=dst, send_sem=ssem.at[kind, c], recv_sem=rsem.at[kind, c],
            device_id=peer, device_id_type=MESH,
        )

    A, B = pl.ds(0, 2), pl.ds(2, 2)
    copies = []
    for c in range(C):
        one = {
            FAR_A: remote(part.at[c, A, far_y], mid_a.at[c], FAR_A, c, {"y": right_y}),
            FAR_B: remote(part.at[c, B, far_y], mid_b.at[c], FAR_B, c, {"y": left_y}),
            SUM_A: remote(mid_a.at[c], from_l.at[c, A], SUM_A, c, {"y": right_y}),
            SUM_B: remote(mid_b.at[c], from_r.at[c, B], SUM_B, c, {"y": left_y}),
            NEAR_B: remote(part.at[c, B, right_y], from_l.at[c, B], NEAR_B, c, {"y": right_y}),
            NEAR_A: remote(part.at[c, A, left_y], from_r.at[c, A], NEAR_A, c, {"y": left_y}),
            XR: remote(feats.at[s, x, c], feats.at[s, x, c], XR, c, {"x": right_x}),
            XL: remote(feats.at[s, x, c], feats.at[s, x, c], XL, c, {"x": left_x}),
            FWD_A: remote(feats.at[s, left_x, c, A], feats.at[s, left_x, c, A], FWD_A, c, {"x": right_x}),
            FWD_B: remote(feats.at[s, right_x, c, B], feats.at[s, right_x, c, B], FWD_B, c, {"x": left_x}),
            OWN_S: remote(feats.at[s, x, c], feats.at[s, x, c], OWN_S, c, {"section": other}),
            LEFT_S: remote(feats.at[s, left_x, c], feats.at[s, left_x, c], LEFT_S, c, {"section": other}),
            RIGHT_S: remote(feats.at[s, right_x, c], feats.at[s, right_x, c], RIGHT_S, c, {"section": other}),
            FAR_SA: remote(feats.at[s, far_x, c, A], feats.at[s, far_x, c, A], FAR_SA, c, {"section": other}),
            FAR_SB: remote(feats.at[s, far_x, c, B], feats.at[s, far_x, c, B], FAR_SB, c, {"section": other}),
        }
        for i, kind in enumerate((Z1, Z2, Z3)):
            to = lax.rem(z + i + 1, 4)
            one[kind] = remote(pooled.at[c, to], feats.at[s, x, c, z], kind, c, {"z": to})
        copies.append(one)

    def start(c, *kinds):
        for kind in kinds:
            copies[c][kind].start()

    def arrive(c, *kinds):
        for kind in kinds:
            copies[c][kind].wait_recv()

    right_z, left_z = lax.rem(z + 1, 4), lax.rem(z + 3, 4)

    def w_copies(k, src, full, row, axis, to):
        return [
            pltpu.make_async_remote_copy(
                src_ref=src.at[i], dst_ref=full.at[row, i], send_sem=wsend.at[k, i], recv_sem=wrecv.at[k, i],
                device_id={axis: to}, device_id_type=MESH,
            )
            for i in range(4)
        ]

    w_y = [w_copies(0, w_a, full_a, y, "y", left_y), w_copies(1, a_left, full_a, left_y, "y", right_y)]
    w_z = [w_copies(2, w_b, full_b, z, "z", left_z), w_copies(3, b_left, full_b, left_z, "z", right_z)]

    def w_start(both, *pieces):
        for i in pieces:
            both[0][i].start()
            both[1][i].start()

    def stage_far(c):
        start(c, FAR_A, FAR_B)

    def stage_sum(c):
        arrive(c, FAR_A)
        mid_a[c] = (mid_a[c].astype(jnp.float32) + part[c, 0:2, right_y].astype(jnp.float32)).astype(jnp.bfloat16)
        start(c, SUM_A)
        arrive(c, FAR_B)
        mid_b[c] = (mid_b[c].astype(jnp.float32) + part[c, 2:4, left_y].astype(jnp.float32)).astype(jnp.bfloat16)
        start(c, SUM_B)
        start(c, NEAR_B, NEAR_A)
        if c + 2 < C:
            stage_far(c + 2)

    def stage_pool(c):
        arrive(c, SUM_A, NEAR_B, SUM_B, NEAR_A)
        total = part[c, :, y].astype(jnp.float32) + from_l[c].astype(jnp.float32) + from_r[c].astype(jnp.float32)
        pooled[c] = total.astype(jnp.bfloat16)
        start(c, Z1, Z3, Z2)
        feats[s, x, c, z] = pooled[c, z]

    def stage_x(c):
        arrive(c, Z1, Z3, Z2)
        start(c, XR, XL, OWN_S)

    def stage_fwd(c):
        arrive(c, XR)
        start(c, FWD_A, LEFT_S)
        arrive(c, XL)
        start(c, FWD_B, RIGHT_S)

    def stage_far_s(c):
        arrive(c, FWD_A)
        start(c, FAR_SA)
        arrive(c, FWD_B)
        start(c, FAR_SB)

    columns = pl.ds(pl.multiple_of(x * 512, 512), 512)
    bias_row = bias[:, columns].astype(jnp.float32)
    scale_row = scale[:, columns].astype(jnp.float32)

    def multiply(first, last, si):
        rows = (last - first) * 128

        @pl.loop(0, 4)
        def _(xi):
            i = si * 4 + xi
            zi, wx = 2 * lax.rem(xi, 2), i // 2
            lhs = jnp.concatenate(
                [jnp.concatenate([feats[si, xi, c, j] for j in range(4)], axis=1) for c in range(first, last)], axis=0
            )
            rhs_a = jnp.concatenate([full_a[yy, zi + zz, wx] for zz in range(2) for yy in range(4)], axis=0)
            acc[0:rows, 0:256] += jnp.dot(lhs, rhs_a, preferred_element_type=jnp.float32)
            rhs_b = jnp.concatenate([full_b[zi + zz, yy, wx] for zz in range(2) for yy in range(4)], axis=0)
            acc[0:rows, 256:512] += jnp.dot(lhs, rhs_b, preferred_element_type=jnp.float32)

    def dense_rows(first, last):
        rows = (last - first) * 128
        acc[0:rows] = jnp.zeros((rows, 512), jnp.float32)
        multiply(first, last, s)
        for c in range(first, last):
            arrive(c, OWN_S, LEFT_S, RIGHT_S, FAR_SA, FAR_SB)
        multiply(first, last, other)

        for k in range(rows // 128):
            h = jnp.maximum(acc[k * 128:(k + 1) * 128] + bias_row, 0.0) * scale_row
            h = h[:, 0:128] + h[:, 128:256] + h[:, 256:384] + h[:, 384:512]
            plog[first + k] = jnp.sum(h.T, axis=0, keepdims=True)

    stage_far(0)
    stage_far(1)
    w_start(w_z, 0, 1)
    full_a[y] = w_a[...]
    full_a[left_y] = a_left[...]
    full_b[z] = w_b[...]
    full_b[left_z] = b_left[...]
    stages = (stage_sum, stage_pool, stage_x, stage_fwd, stage_far_s)
    for step in range(C + len(stages) - 1):
        if step == C + 3:
            for copy in sum(w_y + w_z, []):
                copy.wait_recv()
            dense_rows(0, 3)
        for i, stage in enumerate(stages):
            if 0 <= step - i < C:
                stage(step - i)
        if step == 1:
            w_start(w_z, 2)
        elif step == 2:
            w_start(w_z, 3)
        elif step == 3:
            w_start(w_y, 0, 1, 2, 3)
    dense_rows(3, 4)

    sent = []
    for ds in range(2):
        for dx in range(4):
            if ds == 0 and dx == 0:
                continue
            to_s = s if ds == 0 else other
            to_x = lax.rem(x + dx, 4)
            k = ds * 4 + dx
            copy = pltpu.make_async_remote_copy(
                src_ref=plog.at[to_x], dst_ref=lrecv.at[s * 4 + x], send_sem=lsend.at[k], recv_sem=lrec.at[k],
                device_id={"section": to_s, "x": to_x}, device_id_type=MESH,
            )
            copy.start()
            sent.append(copy)
    lrecv[s * 4 + x] = plog[x]
    for copy in sent:
        copy.wait_recv()
    total = lrecv[0]
    for i in range(1, 8):
        total = total + lrecv[i]
    out[...] = total
    for copy in sent + sum(w_y + w_z, []):
        copy.wait_send()
    for c in range(C):
        for kind in range(KINDS):
            copies[c][kind].wait_send()


def dense(partial, weights, bias, scale):
    bf = jnp.bfloat16
    vmem = pl.BlockSpec(memory_space=pltpu.VMEM)
    return pl.pallas_call(
        dense_kernel,
        out_shape=jax.ShapeDtypeStruct((1, 128), jnp.float32),
        in_specs=[vmem] * 7,
        out_specs=vmem,
        scratch_shapes=[
            pltpu.VMEM((C, 2, 128, 128), bf),
            pltpu.VMEM((C, 2, 128, 128), bf),
            pltpu.VMEM((C, 4, 128, 128), bf),
            pltpu.VMEM((C, 4, 128, 128), bf),
            pltpu.VMEM((C, 4, 128, 128), bf),
            pltpu.VMEM((2, 4, C, 4, 128, 128), bf),
            pltpu.VMEM((384, 512), jnp.float32),
            pltpu.VMEM((C, 1, 128), jnp.float32),
            pltpu.VMEM((8, 1, 128), jnp.float32),
            pltpu.VMEM((4, 4, 4, 64, 256), bf),
            pltpu.VMEM((4, 4, 4, 64, 256), bf),
            pltpu.SemaphoreType.DMA((KINDS, C)),
            pltpu.SemaphoreType.DMA((KINDS, C)),
            pltpu.SemaphoreType.DMA((8,)),
            pltpu.SemaphoreType.DMA((8,)),
            pltpu.SemaphoreType.DMA((4, 4)),
            pltpu.SemaphoreType.DMA((4, 4)),
        ],
        compiler_params=pltpu.CompilerParams(collective_id=1, has_side_effects=True, vmem_limit_bytes=20 << 20),
        cost_estimate=pl.CostEstimate(flops=3 * 10**10, bytes_accessed=10**7, transcendentals=0),
    )(partial.reshape(4, 4, 4, 128, 128), *weights, bias, scale)


ALL = ("section", "x", "z", "y")


def body(indices, pool_len, tables, w_first, b_first, w_out):
    lists, w_a, w_b, tab = front(indices, pool_len, w_first, tables)
    up = [(i, (i + 1) % 4) for i in range(4)]
    weights = [w_a, w_b, lax.ppermute(w_a, "y", up), lax.ppermute(w_b, "z", up)]
    partial = lookup(lists.reshape(SRC, CAP), tab)
    return dense(partial, weights, b_first[None, :], w_out[None, :]).reshape(128)


def solution(mesh):
    grid = Mesh(mesh.devices.reshape(2, 4, 4, 4), ALL)
    dev = ("x", "z", "y")
    placed = (
        P(ALL, None, None),
        P(),
        P(ALL, None),
        P(dev, "section"),
        P("section"),
        P("section"),
    )
    return jax.shard_map(body, mesh=grid, in_specs=placed, out_specs=P(dev), check_vma=False)
```
